256 devices in a mesh: dp: 16 (over y_lo, z), tp: 16 (over y_hi, x, core).
Axes of the slice: x: 4, y: 4 (y_hi: 2, y_lo: 2; y = y_hi * 2 + y_lo), z: 8, core: 2. Of those that a mesh axis runs over, the one named last changes fastest.
Arguments:
- queries: bfloat16 [512, 16, 8192], P(('dp', 'tp')), parts along dimension 0, may hold values from -512 to 512
- kv_cache: bfloat16 [512, 8, 384, 256], P(('dp', 'tp')), parts along dimension 0, may hold values from -18 to 18
- lengths: int32 [512], P(('dp', 'tp')), parts along dimension 0, may hold values from 17 to 384, as said below
- residual: bfloat16 [512, 16, 8192], P(('dp', 'tp')), parts along dimension 0, may hold values from -4 to 4
- out_weight: bfloat16 [8192, 8192], P('tp'), may hold values from -0.0625 to 0.0625
- norm_gain: bfloat16 [8192], replicated, may hold values from 0.25 to 1.75
Outputs:
- hidden: bfloat16 [512, 16, 8192], P(('dp', 'tp')), parts along dimension 0
- normed: bfloat16 [512, 16, 8192], P(('dp', 'tp')), parts along dimension 0
The draws below stay inside these ranges and needn't reach their ends.
There are 16 independent parts, one for each index of `dp`. The reference program is written for one: setup_inputs(seed, part) draws one part's arguments, and reference() takes and returns one part's arrays. A program takes and returns all parts, laid end to end along the dimension named above; an argument that names none is the same for every part. Nothing has to cross between parts.
Inputs may be any that keep to these rules, and one draw needn't show every extreme that they name: `lengths`: some sequence of every part has exactly 384 live slots.
All inputs are finite; a program needn't handle non-finite values.
Results may differ from the reference program's by a relative error of at most 0.015.
Values may be sent and summed in bfloat16 or wider, within the bound.
A program may use at most 128 MiB of HBM per device.

```python
import jax
import jax.numpy as jnp
from jax import lax

D = 8192
HEADS = 64
KV_HEADS = 8
HEAD_DIM = 128
DRAFT = 16
LEN = 384
SEQS = 32
N_TP = 16


def draw_queries(key, part):
    normal_part = jnp.clip(jax.random.normal(jax.random.fold_in(key, 11), (SEQS, DRAFT, HEADS * HEAD_DIM), jnp.float32) * 1.5, -9.0, 9.0)
    return normal_part.astype(jnp.bfloat16)


def draw_kv_cache(key, part):
    shape_all = (SEQS, KV_HEADS, LEN, HEAD_DIM)
    key_part = jnp.clip(jax.random.normal(jax.random.fold_in(key, 21), shape_all, jnp.float32), -6.0, 6.0)
    value_part = jnp.clip(jax.random.normal(jax.random.fold_in(key, 22), shape_all, jnp.float32) * 3.0, -18.0, 18.0)
    return jnp.concatenate([key_part, value_part], axis=-1).astype(jnp.bfloat16)


def draw_lengths(key, part):
    drawn = jax.random.randint(jax.random.fold_in(key, 31), (SEQS,), DRAFT + 1, LEN + 1, dtype=jnp.int32)
    return drawn.at[0].set(LEN)


def draw_residual(key, part):
    row_values = jax.random.normal(jax.random.fold_in(key, 41), (SEQS, DRAFT, D), jnp.float32) * 0.5
    return jnp.clip(row_values, -4.0, 4.0).astype(jnp.bfloat16)


def block_scale(own_key, extent, cuts, smallest, top_value):
    loudness, own = 1.0, jax.random.fold_in(own_key, 6)
    for dim, parts in cuts:
        heights = jnp.exp(jax.random.uniform(jax.random.fold_in(own, dim), (parts,), jnp.float32, smallest / len(cuts), top_value / len(cuts)))
        loudness = loudness * jnp.repeat(heights, extent[dim] // parts).reshape([-1 if axis == dim else 1 for axis in range(len(extent))])
    return loudness


def gaussian(key, extent, width, most, shards=(), kind=jnp.bfloat16):
    gain = block_scale(key, extent, shards, -0.22, 0.18) if shards else 1.0
    entries = jax.random.normal(key, extent, jnp.float32) * width * gain
    return jnp.minimum(jnp.maximum(entries, -most), most).astype(kind)


def setup_inputs(seed: int = 0, part: int = 0) -> dict:
    key_list = jax.random.split(jax.random.key(seed), 7)
    own_keys = jax.random.split(jax.random.fold_in(key_list[6], part), 7)
    return {
        "queries": draw_queries(jax.random.fold_in(jax.random.fold_in(key_list[6], part), 71), part),
        "kv_cache": draw_kv_cache(jax.random.fold_in(jax.random.fold_in(key_list[6], part), 71), part),
        "lengths": draw_lengths(jax.random.fold_in(jax.random.fold_in(key_list[6], part), 71), part),
        "residual": draw_residual(jax.random.fold_in(jax.random.fold_in(key_list[6], part), 71), part),
        "out_weight": gaussian(key_list[4], (HEADS * HEAD_DIM, D), (HEADS * HEAD_DIM) ** -0.5, 0.0625, ((0, 16),)),
        "norm_gain": jnp.clip(1.0 + 0.15 * jax.random.normal(key_list[5], (D,), jnp.float32), 0.25, 1.75).astype(jnp.bfloat16),
    }


def attend(queries, kv_cache, lengths):
    seq_count = queries.shape[0]
    per_group = HEADS // KV_HEADS
    grouped = queries.reshape(seq_count, DRAFT, KV_HEADS, per_group, HEAD_DIM).transpose(0, 2, 3, 1, 4)
    grouped = grouped.reshape(seq_count, KV_HEADS, per_group * DRAFT, HEAD_DIM).astype(jnp.float32)
    key_part = kv_cache[..., :HEAD_DIM].astype(jnp.float32)
    value_part = kv_cache[..., HEAD_DIM:].astype(jnp.float32)
    scores = jnp.einsum('skqd,skld->skql', grouped, key_part) * HEAD_DIM ** (-0.5)
    draft_index = jnp.arange(per_group * DRAFT, dtype=jnp.int32) % DRAFT
    visible = lengths[:, None, None, None] - DRAFT + 1 + draft_index[None, None, :, None]
    position = jnp.arange(LEN, dtype=jnp.int32)
    allowed = position[None, None, None, :] < visible
    scores = jnp.where(allowed, scores, -1e+30)
    peak = lax.optimization_barrier(jnp.max(scores, axis=-1, keepdims=True))
    raised = jnp.exp(scores - peak)
    totals = lax.optimization_barrier(jnp.sum(raised, axis=-1, keepdims=True))
    weights = (raised / totals).astype(jnp.bfloat16)
    attended = jnp.einsum('skql,skld->skqd', weights.astype(jnp.float32), value_part).astype(jnp.bfloat16)
    attended = attended.reshape(seq_count, KV_HEADS, per_group, DRAFT, HEAD_DIM).transpose(0, 3, 1, 2, 4)
    return attended.reshape(seq_count, DRAFT, HEADS * HEAD_DIM)

def reference(queries, kv_cache, lengths, residual, out_weight, norm_gain):
    attended = attend(queries, kv_cache, lengths)
    flat_rows = attended.reshape(SEQS * DRAFT, HEADS * HEAD_DIM)
    columns = HEADS * HEAD_DIM // N_TP
    projected = jnp.zeros((SEQS * DRAFT, D), jnp.float32)
    for shard in range(N_TP):
        partial_term = jnp.dot(flat_rows[:, shard * columns:(shard + 1) * columns], out_weight[shard * columns:(shard + 1) * columns], preferred_element_type=jnp.float32)
        projected = projected + lax.optimization_barrier(partial_term.astype(jnp.bfloat16)).astype(jnp.float32)
    summed = residual.astype(jnp.float32) + projected.reshape(SEQS, DRAFT, D)
    hidden = summed.astype(jnp.bfloat16)
    scales = lax.rsqrt(lax.optimization_barrier(jnp.mean(summed * summed, axis=-1, keepdims=True)) + 1e-05)
    normed = (summed * scales * norm_gain.astype(jnp.float32)).astype(jnp.bfloat16)
    return (hidden, normed)
```

```python
import functools

import jax
import jax.numpy as jnp
from jax import lax
from jax.experimental import pallas as pl
from jax.experimental.pallas import tpu as pltpu
from jax.sharding import PartitionSpec as P

KV_HEADS = 8
HEAD_DIM = 128
GROUP = 8
DRAFT = 16
TILE = 256
MESH = pl.DeviceIdType.MESH
F32 = jnp.float32
BF16 = jnp.bfloat16

CHUNKS = ((1, 2), (2, 2), (1, 2), (2, 2), (1, 2), (2, 2), (1, 3), (2, 1))

FAR_UP, FAR_DOWN, NEAR_UP, NEAR_DOWN, SUM_UP, SUM_DOWN, ACROSS = range(7)

ORDER = (
    ("d", 0), ("d", 2), ("s", 1), ("d", 4), ("z", 0), ("d", 1), ("s", 3), ("d", 6),
    ("z", 2), ("d", 3), ("s", 5), ("z", 4), ("f", 1), ("d", 5), ("s", 7), ("f", 0),
    ("z", 6), ("d", 7), ("f", 3), ("f", 2), ("f", 5), ("f", 4), ("f", 7), ("f", 6),
)


def kernel(
    dp_half,
    lengths,
    q_hbm,
    kv_hbm,
    res_hbm,
    w_hbm,
    gain,
    hid_hbm,
    norm_hbm,
    q,
    kv,
    res,
    w,
    stage,
    att,
    part,
    far_up,
    far_down,
    from_down,
    from_up,
    across,
    total,
    hid,
    norm,
    in_sem,
    kv_sem,
    w_sem,
    swap_send,
    swap_recv,
    a_send,
    a_recv,
    r_send,
    r_recv,
    out_sem,
):
    seqs = q.shape[0]
    rows = seqs * DRAFT
    width = part.shape[3]
    dp, tp = lax.axis_index("dp"), lax.axis_index("tp")
    y_hi, x, core = tp // 8, (tp // 2) % 4, tp % 2

    def peer(dx, dy):
        return (
            (dp + dy * dp_half) % (2 * dp_half),
            ((y_hi + dy) % 2) * 8 + ((x + dx) % 4) * 2 + core,
        )

    sibling = (dp, tp + 1 - 2 * core)

    def turn(i):
        h = i // 2
        return (2 - h * (h + 1) // 2) % 4, (i + 1) % 2

    chunks, start = [], 0
    for kind, share in CHUNKS:
        size = share * width // 16
        chunks.append((kind, start, size))
        start += size

    q_copy = pltpu.make_async_copy(q_hbm, q, in_sem.at[0])
    q_copy.start()

    def kv_head(i):
        dx, dy = turn(i)
        return ((y_hi + dy) % 2) * 4 + (x + dx) % 4

    def kv_copy(i):
        return pltpu.make_async_copy(kv_hbm.at[:, kv_head(i)], kv.at[i], kv_sem.at[i])

    for i in range(KV_HEADS):
        kv_copy(i).start()

    barrier = pltpu.get_barrier_semaphore()
    friends = [sibling] + [peer(i % 4, i // 4) for i in range(1, 8)]
    for friend in friends:
        pl.semaphore_signal(barrier, inc=1, device_id=friend, device_id_type=MESH)

    res_copy = pltpu.make_async_copy(res_hbm, res, in_sem.at[1])
    res_copy.start()

    def w_copy(j):
        cols = pl.ds(chunks[j][1], chunks[j][2])
        return pltpu.make_async_copy(w_hbm.at[:, cols], w.at[0, :, cols], w_sem.at[j])

    def swap_copy(j):
        cols = pl.ds(chunks[j][1], chunks[j][2])
        return pltpu.make_async_remote_copy(
            w_hbm.at[:, cols],
            w.at[1, :, cols],
            swap_send.at[j],
            swap_recv.at[j],
            device_id=sibling,
            device_id_type=MESH,
        )

    pl.semaphore_wait(barrier, len(friends))
    for j in range(len(chunks)):
        swap_copy(j).start()
    for j in range(len(chunks)):
        w_copy(j).start()

    def att_copy(i):
        dx, dy = turn(i)
        return pltpu.make_async_remote_copy(
            stage.at[i],
            att.at[dy, (4 - dx) % 4],
            a_send.at[i],
            a_recv.at[i],
            device_id=peer(dx, dy),
            device_id_type=MESH,
        )

    draft = lax.broadcasted_iota(jnp.int32, (GROUP * DRAFT, kv.shape[2]), 0) % DRAFT
    slot = lax.broadcasted_iota(jnp.int32, (GROUP * DRAFT, kv.shape[2]), 1)
    ahead = slot - draft
    q_copy.wait()

    def one_head(i, carry):
        k = kv_head(i)
        kv_copy(i).wait()
        cols = pl.ds(pl.multiple_of(k * GROUP * HEAD_DIM, GROUP * HEAD_DIM), GROUP * HEAD_DIM)
        for s in range(seqs):
            heads = q[s, :, cols]
            grouped = jnp.concatenate(
                [heads[:, g * HEAD_DIM : (g + 1) * HEAD_DIM] for g in range(GROUP)], axis=0
            )
            keys = kv[i, s, :, :HEAD_DIM]
            values = kv[i, s, :, HEAD_DIM:]
            scores = lax.dot_general(
                grouped, keys, (((1,), (1,)), ((), ())), preferred_element_type=F32
            ) * (HEAD_DIM ** (-0.5))
            scores = jnp.where(ahead < lengths[s] - DRAFT + 1, scores, -1e30)
            peak = jnp.max(scores, axis=-1, keepdims=True)
            raised = jnp.exp(scores - peak)
            sums = jnp.sum(raised, axis=-1, keepdims=True)
            out = jnp.dot(raised.astype(BF16), values, preferred_element_type=F32)
            out = (out / sums).astype(BF16)
            stage[i, s * DRAFT : (s + 1) * DRAFT, :] = jnp.concatenate(
                [out[g * DRAFT : (g + 1) * DRAFT] for g in range(GROUP)], axis=1
            )

        @pl.when(i < KV_HEADS - 1)
        def _():
            att_copy(i).start()

        return carry

    lax.fori_loop(0, KV_HEADS, one_head, 0)
    att[0, 0] = stage[KV_HEADS - 1]

    def remote(j, which, source, target, device):
        return pltpu.make_async_remote_copy(
            source,
            target,
            r_send.at[j, which],
            r_recv.at[j, which],
            device_id=device,
            device_id_type=MESH,
        )

    low, high = pl.ds(0, rows // 2), pl.ds(rows // 2, rows // 2)
    up, down, over = peer(1, 0), peer(3, 0), peer(0, 1)

    def copies(j):
        kind, begin, size = chunks[j]
        cols = pl.ds(begin, size)
        if kind == 1:
            pairs = {
                FAR_UP: (part.at[0, 2, :, cols], far_up.at[:, cols], up),
                FAR_DOWN: (part.at[1, 2, :, cols], far_down.at[:, cols], down),
                NEAR_UP: (part.at[1, 1, :, cols], from_down.at[1, :, cols], up),
                NEAR_DOWN: (part.at[0, 3, :, cols], from_up.at[0, :, cols], down),
                SUM_UP: (part.at[0, 1, :, cols], from_down.at[0, :, cols], up),
                SUM_DOWN: (part.at[1, 3, :, cols], from_up.at[1, :, cols], down),
                ACROSS: (part.at[1, 0, :, cols], across.at[0, :, cols], over),
            }
        else:
            pairs = {
                FAR_UP: (part.at[0, 2, low, cols], far_up.at[low, cols], up),
                FAR_DOWN: (part.at[0, 2, high, cols], far_down.at[high, cols], down),
                NEAR_UP: (part.at[0, 1, high, cols], from_down.at[0, high, cols], up),
                NEAR_DOWN: (part.at[0, 3, low, cols], from_up.at[0, low, cols], down),
                SUM_UP: (part.at[0, 1, low, cols], from_down.at[0, low, cols], up),
                SUM_DOWN: (part.at[0, 3, high, cols], from_up.at[0, high, cols], down),
                ACROSS: (part.at[1, :, :, cols], across.at[:, :, cols], over),
            }
        return {which: remote(j, which, *pair) for which, pair in pairs.items()}

    for i in range(KV_HEADS - 1):
        att_copy(i).wait_recv()
    for j, (kind, begin, size) in enumerate(chunks):
        w_copy(j).wait()
        swap_copy(j).wait_recv()

        def tile(n, carry, begin=begin):
            cols = pl.ds(pl.multiple_of(begin + n * TILE, TILE), TILE)
            half = w.shape[1]
            own = pl.ds(pl.multiple_of(core * half, half), half)
            other = pl.ds(pl.multiple_of((1 - core) * half, half), half)
            count = 8 * rows
            out = jnp.dot(
                att[:, :, :, own].reshape(count, half), w[0, :, cols], preferred_element_type=F32
            ) + jnp.dot(
                att[:, :, :, other].reshape(count, half), w[1, :, cols], preferred_element_type=F32
            )
            part[:, :, :, cols] = out.astype(BF16).reshape(2, 4, rows, TILE)
            return carry

        lax.fori_loop(0, size // TILE, tile, 0)
        sends = copies(j)
        first = (FAR_UP, FAR_DOWN, NEAR_UP, NEAR_DOWN) if kind == 1 else (ACROSS,)
        for which in first:
            sends[which].start()

    def add(target, *terms):
        value = part[target].astype(F32)
        for ref, index in terms:
            value = value + ref[index].astype(F32)
        part[target] = value.astype(BF16)

    every = slice(None)
    top, bottom = slice(0, rows // 2), slice(rows // 2, rows)
    res_copy.wait()
    squares = []

    def hidden_copy(j):
        cols = pl.ds(chunks[j][1], chunks[j][2])
        return pltpu.make_async_copy(hid.at[:, :, cols], hid_hbm.at[:, :, cols], out_sem.at[j])

    for step, j in ORDER:
        kind, begin, size = chunks[j]
        cols = slice(begin, begin + size)
        sends = copies(j)
        if step == "s":
            sends[ACROSS].wait_recv()
            for dx in (2, 1, 3):
                add((0, dx, every, cols), (across, (dx, every, cols)))
            for which in (FAR_UP, FAR_DOWN, NEAR_UP, NEAR_DOWN):
                sends[which].start()
        elif step == "d":
            sends[FAR_UP].wait_recv()
            lines = every if kind == 1 else top
            add((0, 1, lines, cols), (far_up, (lines, cols)))
            sends[SUM_UP].start()
            sends[FAR_DOWN].wait_recv()
            lines = every if kind == 1 else bottom
            add((1 if kind == 1 else 0, 3, lines, cols), (far_down, (lines, cols)))
            sends[SUM_DOWN].start()
        elif step == "z":
            for which in (NEAR_UP, NEAR_DOWN, SUM_UP, SUM_DOWN):
                sends[which].wait_recv()
            add(
                (1, 0, every, cols),
                (from_down, (1, every, cols)),
                (from_up, (1, every, cols)),
            )
            sends[ACROSS].start()
        else:
            if kind == 1:
                sends[ACROSS].wait_recv()
            else:
                for which in (NEAR_UP, NEAR_DOWN, SUM_UP, SUM_DOWN):
                    sends[which].wait_recv()
            value = (
                part[0, 0, :, cols].astype(F32)
                + from_down[0, :, cols].astype(F32)
                + from_up[0, :, cols].astype(F32)
                + across[0, :, cols].astype(F32)
                + res[:, :, cols].astype(F32).reshape(rows, size)
            )
            total[:, cols] = value
            hid[:, :, cols] = value.astype(BF16).reshape(seqs, DRAFT, size)
            hidden_copy(j).start()
            squares.append(jnp.sum(value * value, axis=-1, keepdims=True))

    scale = lax.rsqrt(sum(squares) / width + 1e-5)
    for j, (kind, begin, size) in enumerate(chunks):
        cols = slice(begin, begin + size)
        value = total[:, cols] * scale * gain[:, cols].astype(F32)
        norm[:, :, cols] = value.astype(BF16).reshape(seqs, DRAFT, size)
    norm_copy = pltpu.make_async_copy(norm, norm_hbm, in_sem.at[2])
    norm_copy.start()

    for i in range(KV_HEADS - 1):
        att_copy(i).wait_send()
    for j in range(len(chunks)):
        swap_copy(j).wait_send()
        for copy in copies(j).values():
            copy.wait_send()
        hidden_copy(j).wait()
    norm_copy.wait()


def solution(mesh):
    dp_half = mesh.shape["dp"] // 2

    def on_device(queries, kv_cache, lengths, residual, out_weight, norm_gain):
        seqs = queries.shape[0]
        rows = seqs * DRAFT
        depth, width = out_weight.shape
        slots = kv_cache.shape[2]
        n = len(CHUNKS)
        anywhere = pl.BlockSpec(memory_space=pl.ANY)
        dma = pltpu.SemaphoreType.DMA
        return pl.pallas_call(
            functools.partial(kernel, dp_half),
            out_shape=(jax.ShapeDtypeStruct((seqs, DRAFT, width), BF16),) * 2,
            in_specs=[pl.BlockSpec(memory_space=pltpu.SMEM)]
            + [anywhere] * 4
            + [pl.BlockSpec(memory_space=pltpu.VMEM)],
            out_specs=(anywhere, anywhere),
            scratch_shapes=[
                pltpu.VMEM(queries.shape, BF16),
                pltpu.VMEM((KV_HEADS, seqs, slots, 2 * HEAD_DIM), BF16),
                pltpu.VMEM(residual.shape, BF16),
                pltpu.VMEM((2, depth, width), BF16),
                pltpu.VMEM((KV_HEADS, rows, GROUP * HEAD_DIM), BF16),
                pltpu.VMEM((2, 4, rows, GROUP * HEAD_DIM), BF16),
                pltpu.VMEM((2, 4, rows, width), BF16),
                pltpu.VMEM((rows, width), BF16),
                pltpu.VMEM((rows, width), BF16),
                pltpu.VMEM((2, rows, width), BF16),
                pltpu.VMEM((2, rows, width), BF16),
                pltpu.VMEM((4, rows, width), BF16),
                pltpu.VMEM((rows, width), F32),
                pltpu.VMEM(residual.shape, BF16),
                pltpu.VMEM(residual.shape, BF16),
                dma((3,)),
                dma((KV_HEADS,)),
                dma((n,)),
                dma((n,)),
                dma((n,)),
                dma((KV_HEADS,)),
                dma((KV_HEADS,)),
                dma((n, 7)),
                dma((n, 7)),
                dma((n,)),
            ],
            compiler_params=pltpu.CompilerParams(
                collective_id=0, has_side_effects=True, vmem_limit_bytes=56 * 1024 * 1024
            ),
        )(lengths, queries, kv_cache, residual, out_weight, norm_gain.reshape(1, -1))

    seq = P(("dp", "tp"))
    return jax.shard_map(
        on_device,
        mesh=mesh,
        in_specs=(seq, seq, seq, seq, P("tp"), P()),
        out_specs=(seq, seq),
        check_vma=False,
    )
```

```python
import functools

import jax
import jax.numpy as jnp
from jax import lax
from jax.experimental import pallas as pl
from jax.experimental.pallas import tpu as pltpu
from jax.sharding import PartitionSpec as P

KV_HEADS = 8
HEAD_DIM = 128
GROUP = 8
DRAFT = 16
TILE = 512
VMEM_LIMIT = 54735667
MESH = pl.DeviceIdType.MESH
F32 = jnp.float32
BF16 = jnp.bfloat16

CHUNKS = (
    (1, 0, 16, 0, 2),
    (2, 0, 16, 9, 2),
    (1, 16, 16, 0, 2),
    (2, 16, 16, 9, 2),
    (1, 0, 16, 2, 2),
    (1, 16, 16, 2, 2),
    (2, 0, 32, 11, 2),
    (1, 0, 32, 4, 2),
    (2, 0, 32, 13, 2),
    (1, 0, 32, 6, 2),
    (1, 0, 32, 8, 1),
    (2, 0, 32, 15, 1),
)
PIECES = ((0, 2), (9, 2), (2, 2), (11, 2), (4, 2), (13, 2), (6, 2), (15, 1), (8, 1))

FAR_UP, FAR_DOWN, NEAR_UP, NEAR_DOWN, SUM_UP, SUM_DOWN, ACROSS = range(7)

PLAN = (
    ("m", 0), ("x", 0), ("m", 1), ("y", 1), ("e", 0), ("m", 4), ("x", 4), ("e", 4), ("m", 3),
    ("y", 3), ("d", 0), ("m", 5), ("e", 5), ("x", 5), ("m", 2), ("e", 2), ("m", 6), ("s", 1),
    ("x", 2), ("y", 6), ("d", 4), ("m", 7), ("x", 7), ("e", 7), ("m", 8), ("y", 8), ("d", 5),
    ("z", 0), ("m", 9), ("x", 9), ("m", 11), ("y", 11), ("d", 7), ("e", 9), ("m", 10), ("d", 9),
    ("x", 10), ("d", 1), ("d", 2), ("s", 3), ("e", 1), ("e", 10), ("z", 7), ("z", 5), ("s", 6),
    ("d", 10), ("s", 8), ("e", 8), ("d", 3), ("z", 4), ("z", 9), ("s", 11), ("z", 2), ("f", 1),
    ("e", 3), ("e", 6), ("z", 10), ("d", 6), ("d", 8), ("e", 11), ("f", 5), ("d", 11), ("f", 9),
    ("f", 6), ("f", 7), ("f", 2), ("f", 4), ("f", 8), ("f", 3), ("f", 10), ("f", 0), ("f", 11),
)


def kernel(
    dp_half,
    lengths,
    q_hbm,
    kv_hbm,
    res_hbm,
    w_hbm,
    hid,
    total_0,
    total_1,
    scale,
    q,
    kv,
    res,
    w,
    stage,
    att,
    part,
    far_up,
    far_down,
    from_down,
    from_up,
    across,
    in_sem,
    q_sem,
    kv_sem,
    w_sem,
    swap_send,
    swap_recv,
    a_send,
    a_recv,
    r_send,
    r_recv,
):
    seqs = q.shape[0]
    width = part.shape[3]
    unit = width // 16
    dp, tp = lax.axis_index("dp"), lax.axis_index("tp")
    y_hi, x, core = tp // 8, (tp // 2) % 4, tp % 2

    def peer(dx, dy):
        return (
            (dp + dy * dp_half) % (2 * dp_half),
            ((y_hi + dy) % 2) * 8 + ((x + dx) % 4) * 2 + core,
        )

    sibling = (dp, tp + 1 - 2 * core)

    def turn(i):
        h = i % 4
        return (2 - h * (h + 1) // 2) % 4, 1 - i // 4

    def kv_head(i):
        dx, dy = turn(i)
        return ((y_hi + dy) % 2) * 4 + (x + dx) % 4

    def q_copy(s, i):
        wide = GROUP * HEAD_DIM
        cols = pl.ds(pl.multiple_of(kv_head(i) * wide, wide), wide)
        return pltpu.make_async_copy(q_hbm.at[s, :, cols], q.at[s, i], q_sem.at[s, i])

    def kv_copy(s, i):
        return pltpu.make_async_copy(kv_hbm.at[s, kv_head(i)], kv.at[s, i], kv_sem.at[s, i])

    def w_copy(j):
        cols = pl.ds(PIECES[j][0] * unit, PIECES[j][1] * unit)
        return pltpu.make_async_copy(w_hbm.at[:, cols], w.at[0, :, cols], w_sem.at[j])

    def swap_copy(j):
        cols = pl.ds(PIECES[j][0] * unit, PIECES[j][1] * unit)
        return pltpu.make_async_remote_copy(
            w_hbm.at[:, cols],
            w.at[1, :, cols],
            swap_send.at[j],
            swap_recv.at[j],
            device_id=sibling,
            device_id_type=MESH,
        )

    barrier = pltpu.get_barrier_semaphore()
    friends = [sibling] + [peer(i % 4, i // 4) for i in range(1, 8)]
    for friend in friends:
        pl.semaphore_signal(barrier, inc=1, device_id=friend, device_id_type=MESH)
    for i in range(KV_HEADS):
        q_copy(0, i).start()
        kv_copy(0, i).start()
    res_copy = pltpu.make_async_copy(res_hbm, res, in_sem.at[0])

    def att_copy(s, i):
        dx, dy = turn(i)
        return pltpu.make_async_remote_copy(
            stage.at[s, i],
            att.at[dy, (4 - dx) % 4, pl.ds(s * DRAFT, DRAFT)],
            a_send.at[s, i],
            a_recv.at[s, i],
            device_id=peer(dx, dy),
            device_id_type=MESH,
        )

    slots = kv.shape[3 - 1]
    draft = lax.broadcasted_iota(jnp.int32, (GROUP * DRAFT, slots), 0) % DRAFT
    slot = lax.broadcasted_iota(jnp.int32, (GROUP * DRAFT, slots), 1)
    ahead = slot - draft

    def attend(s, heads):
        for i in heads:
            q_copy(s, i).wait()
            kv_copy(s, i).wait()
        for i in heads:
            own = q[s, i]
            grouped = jnp.concatenate(
                [own[:, g * HEAD_DIM : (g + 1) * HEAD_DIM] for g in range(GROUP)], axis=0
            )
            keys = kv[s, i, :, :HEAD_DIM]
            values = kv[s, i, :, HEAD_DIM:]
            scores = lax.dot_general(
                grouped, keys, (((1,), (1,)), ((), ())), preferred_element_type=F32
            ) * (HEAD_DIM ** (-0.5))
            scores = jnp.where(ahead < lengths[s] - DRAFT + 1, scores, -1e30)
            raised = jnp.exp(scores - jnp.max(scores, axis=-1, keepdims=True))
            sums = jnp.sum(raised, axis=-1, keepdims=True)
            out = jnp.dot(raised.astype(BF16), values, preferred_element_type=F32)
            out = (out / sums).astype(BF16)
            stage[s, i] = jnp.concatenate(
                [out[g * DRAFT : (g + 1) * DRAFT] for g in range(GROUP)], axis=1
            )

    def some_heads(s, count):
        def body(h, carry):
            heads = [count * h + n for n in range(count)]
            attend(s, heads)
            for n in range(count - 1):
                att_copy(s, heads[n]).start()

            @pl.when(h < KV_HEADS // count - 1)
            def _():
                att_copy(s, heads[count - 1]).start()

            return carry

        return body

    with jax.named_scope("heads#s=0a"):
        attend(0, (0, 1))
    for s in range(1, seqs):
        for i in range(KV_HEADS):
            q_copy(s, i).start()
            kv_copy(s, i).start()
    with jax.named_scope("barrier"):
        pl.semaphore_wait(barrier, len(friends))
    for i in (0, 1):
        att_copy(0, i).start()
    for j in range(len(PIECES)):
        swap_copy(j).start()
        w_copy(j).start()
    res_copy.start()
    with jax.named_scope("heads#s=0"):
        lax.fori_loop(1, KV_HEADS // 2, some_heads(0, 2), 0)
    for s in range(1, seqs):
        with jax.named_scope("heads#s=1"):
            lax.fori_loop(0, KV_HEADS // 4, some_heads(s, 4), 0)
    for s in range(seqs):
        att[0, 0, s * DRAFT : (s + 1) * DRAFT] = stage[s, KV_HEADS - 1]

    up, down, over = peer(1, 0), peer(3, 0), peer(0, 1)

    def area(c):
        kind, row, count, begin, size = CHUNKS[c]
        return kind, slice(row, row + count), slice(begin * unit, (begin + size) * unit)

    def halves(c):
        kind, row, count, begin, size = CHUNKS[c]
        mid, low, high = (begin * unit + size * unit // 2), begin * unit, (begin + size) * unit
        if count == seqs * DRAFT:
            half = count // 2
            return (slice(0, half), slice(low, high)), (slice(half, count), slice(low, high))
        lines = slice(row, row + count)
        return (lines, slice(low, mid)), (lines, slice(mid, high))

    def copies(c):
        kind, lines, cols = area(c)
        if kind == 1:
            pairs = {
                FAR_UP: (part.at[0, 2, lines, cols], far_up.at[lines, cols], up),
                FAR_DOWN: (part.at[1, 2, lines, cols], far_down.at[lines, cols], down),
                NEAR_UP: (part.at[1, 1, lines, cols], from_down.at[1, lines, cols], up),
                NEAR_DOWN: (part.at[0, 3, lines, cols], from_up.at[0, lines, cols], down),
                SUM_UP: (part.at[0, 1, lines, cols], from_down.at[0, lines, cols], up),
                SUM_DOWN: (part.at[1, 3, lines, cols], from_up.at[1, lines, cols], down),
                ACROSS: (part.at[1, 0, lines, cols], across.at[0, lines, cols], over),
            }
        else:
            one, two = halves(c)
            pairs = {
                FAR_UP: (part.at[0, 2, *one], far_up.at[*one], up),
                FAR_DOWN: (part.at[0, 2, *two], far_down.at[*two], down),
                NEAR_UP: (part.at[0, 1, *two], from_down.at[0, *two], up),
                NEAR_DOWN: (part.at[0, 3, *one], from_up.at[0, *one], down),
                SUM_UP: (part.at[0, 1, *one], from_down.at[0, *one], up),
                SUM_DOWN: (part.at[0, 3, *two], from_up.at[0, *two], down),
                ACROSS: (part.at[1, :, lines, cols], across.at[:, lines, cols], over),
            }

        def build(which):
            source, target, device = pairs[which]
            return pltpu.make_async_remote_copy(
                source,
                target,
                r_send.at[c, which],
                r_recv.at[c, which],
                device_id=device,
                device_id_type=MESH,
            )

        return build

    def add(target, *terms):
        value = part[target].astype(F32)
        for ref, index in terms:
            value = value + ref[index].astype(F32)
        part[target] = value.astype(BF16)

    arrived, loaded = set(), set()
    squares = [0.0] * seqs

    def product(c):
        kind, row, count, begin, size = CHUNKS[c]
        for s in range(row // DRAFT, (row + count) // DRAFT):
            if s not in arrived:
                arrived.add(s)
                with jax.named_scope(f"rows#s={s}"):
                    for i in range(KV_HEADS - 1):
                        att_copy(s, i).wait_recv()
        for j, (first, extent) in enumerate(PIECES):
            if j not in loaded and first < begin + size and begin < first + extent:
                loaded.add(j)
                with jax.named_scope(f"weights#j={j}"):
                    w_copy(j).wait()
                    swap_copy(j).wait_recv()

        def tile(n, carry):
            cols = pl.ds(pl.multiple_of(begin * unit + n * TILE, TILE), TILE)
            half = w.shape[1]
            own = pl.ds(pl.multiple_of(core * half, half), half)
            other = pl.ds(pl.multiple_of((1 - core) * half, half), half)
            lines = slice(row, row + count)
            out = jnp.dot(
                att[:, :, lines, own].reshape(8 * count, half),
                w[0, :, cols],
                preferred_element_type=F32,
            ) + jnp.dot(
                att[:, :, lines, other].reshape(8 * count, half),
                w[1, :, cols],
                preferred_element_type=F32,
            )
            part[:, :, lines, cols] = out.astype(BF16).reshape(2, 4, count, TILE)
            return carry

        lax.fori_loop(0, size * unit // TILE, tile, 0)

    def finish(c):
        kind, lines, cols = area(c)
        value = (
            part[0, 0, lines, cols].astype(F32)
            + from_down[0, lines, cols].astype(F32)
            + from_up[0, lines, cols].astype(F32)
            + across[0, lines, cols].astype(F32)
        )
        for n, s in enumerate(range(lines.start // DRAFT, lines.stop // DRAFT)):
            here = value[n * DRAFT : (n + 1) * DRAFT] + res[s, :, cols].astype(F32)
            (total_0, total_1)[s][:, cols] = here
            hid[s, :, cols] = here.astype(BF16)
            squares[s] = squares[s] + jnp.sum(here * here, axis=-1, keepdims=True)

    def advance(step, c):
        kind, lines, cols = area(c)
        build = copies(c)
        every = slice(None)
        if step == "m":
            product(c)
        elif step == "x":
            build(FAR_UP).start()
            build(FAR_DOWN).start()
        elif step == "e":
            build(NEAR_UP).start()
            build(NEAR_DOWN).start()
        elif step == "y":
            build(ACROSS).start()
        elif step == "s":
            build(ACROSS).wait_recv()
            add((0, 2, lines, cols), (across, (2, lines, cols)))
            build(FAR_UP).start()
            build(FAR_DOWN).start()
            for dx in (1, 3):
                add((0, dx, lines, cols), (across, (dx, lines, cols)))
        elif step == "d":
            one, two = halves(c) if kind == 2 else ((lines, cols), (lines, cols))
            build(FAR_UP).wait_recv()
            add((0, 1, *one), (far_up, one))
            build(SUM_UP).start()
            build(FAR_DOWN).wait_recv()
            add((0 if kind == 2 else 1, 3, *two), (far_down, two))
            build(SUM_DOWN).start()
        elif step == "z":
            for which in (NEAR_UP, NEAR_DOWN, SUM_UP, SUM_DOWN):
                build(which).wait_recv()
            add((1, 0, lines, cols), (from_down, (1, lines, cols)), (from_up, (1, lines, cols)))
            build(ACROSS).start()
        else:
            waits = (ACROSS,) if kind == 1 else (NEAR_UP, NEAR_DOWN, SUM_UP, SUM_DOWN)
            for which in waits:
                build(which).wait_recv()
            finish(c)

    res_copy.wait()
    for step, c in PLAN:
        with jax.named_scope(f"{step}#c={c}"):
            advance(step, c)

    with jax.named_scope("scale"):
        for s in range(seqs):
            lane = lax.rsqrt(squares[s] / width + 1e-5)
            scale[s * DRAFT : (s + 1) * DRAFT, :] = jnp.broadcast_to(lane, (DRAFT, 128))

    with jax.named_scope("drain"):
        for s in range(seqs):
            for i in range(KV_HEADS - 1):
                att_copy(s, i).wait_send()
        for j in range(len(PIECES)):
            swap_copy(j).wait_send()
        for c in range(len(CHUNKS)):
            for which in range(7):
                copies(c)(which).wait_send()


def norm_kernel(hid, total_0, total_1, scale, gain, hid_hbm, norm_hbm, norm, sems):
    hid_copy = pltpu.make_async_copy(hid, hid_hbm, sems.at[0])
    hid_copy.start()
    seqs, width = norm.shape[0], norm.shape[2]
    pieces = 4
    size = width // pieces

    def norm_copy(n):
        cols = pl.ds(n * size, size)
        return pltpu.make_async_copy(
            norm.at[:, :, cols], norm_hbm.at[:, :, cols], sems.at[1 + n]
        )

    for n in range(pieces):
        cols = slice(n * size, (n + 1) * size)
        gains = gain[cols].astype(F32).reshape(1, size)
        for s, total in enumerate((total_0, total_1)):
            lane = scale[s * DRAFT : (s + 1) * DRAFT, 0:1]
            norm[s, :, cols] = (total[:, cols] * lane * gains).astype(BF16)
        norm_copy(n).start()
    hid_copy.wait()
    for n in range(pieces):
        norm_copy(n).wait()


def solution(mesh):
    dp_half = mesh.shape["dp"] // 2

    def on_device(queries, kv_cache, lengths, residual, out_weight, norm_gain):
        seqs = queries.shape[0]
        rows = seqs * DRAFT
        depth, width = out_weight.shape
        slots = kv_cache.shape[2]
        chunks, pieces = len(CHUNKS), len(PIECES)
        hbm = pl.BlockSpec(memory_space=pltpu.HBM)
        vmem = pl.BlockSpec(memory_space=pltpu.VMEM)
        dma = pltpu.SemaphoreType.DMA
        sums = pl.pallas_call(
            functools.partial(kernel, dp_half),
            out_shape=(
                jax.ShapeDtypeStruct((seqs, DRAFT, width), BF16),
                jax.ShapeDtypeStruct((DRAFT, width), F32),
                jax.ShapeDtypeStruct((DRAFT, width), F32),
                jax.ShapeDtypeStruct((rows, 128), F32),
            ),
            in_specs=[pl.BlockSpec(memory_space=pltpu.SMEM)] + [hbm] * 4,
            out_specs=(vmem,) * 4,
            scratch_shapes=[
                pltpu.VMEM((seqs, KV_HEADS, DRAFT, GROUP * HEAD_DIM), BF16),
                pltpu.VMEM((seqs, KV_HEADS, slots, 2 * HEAD_DIM), BF16),
                pltpu.VMEM(residual.shape, BF16),
                pltpu.VMEM((2, depth, width), BF16),
                pltpu.VMEM((seqs, KV_HEADS, DRAFT, GROUP * HEAD_DIM), BF16),
                pltpu.VMEM((2, 4, rows, GROUP * HEAD_DIM), BF16),
                pltpu.VMEM((2, 4, rows, width), BF16),
                pltpu.VMEM((rows, width), BF16),
                pltpu.VMEM((rows, width), BF16),
                pltpu.VMEM((2, rows, width), BF16),
                pltpu.VMEM((2, rows, width), BF16),
                pltpu.VMEM((4, rows, width), BF16),
                dma((1,)),
                dma((seqs, KV_HEADS)),
                dma((seqs, KV_HEADS)),
                dma((pieces,)),
                dma((pieces,)),
                dma((pieces,)),
                dma((seqs, KV_HEADS)),
                dma((seqs, KV_HEADS)),
                dma((chunks, 7)),
                dma((chunks, 7)),
            ],
            compiler_params=pltpu.CompilerParams(
                collective_id=0, has_side_effects=True, vmem_limit_bytes=VMEM_LIMIT
            ),
        )(lengths, queries, kv_cache, residual, out_weight)
        return pl.pallas_call(
            norm_kernel,
            out_shape=(jax.ShapeDtypeStruct((seqs, DRAFT, width), BF16),) * 2,
            in_specs=[vmem] * 5,
            out_specs=(hbm, hbm),
            scratch_shapes=[pltpu.VMEM((seqs, DRAFT, width), BF16), dma((5,))],
            compiler_params=pltpu.CompilerParams(vmem_limit_bytes=4 * 1024 * 1024),
        )(*sums, norm_gain)

    seq = P(("dp", "tp"))
    return jax.shard_map(
        on_device,
        mesh=mesh,
        in_specs=(seq, seq, seq, seq, P("tp"), P()),
        out_specs=(seq, seq),
        check_vma=False,
    )
```

```python
import functools

import jax
import jax.numpy as jnp
from jax import lax
from jax.experimental import pallas as pl
from jax.experimental.pallas import tpu as pltpu
from jax.sharding import PartitionSpec as P

KV_HEADS = 8
HEAD_DIM = 128
GROUP = 8
DRAFT = 16
TILE = 512
VMEM_LIMIT = 54735667
MESH = pl.DeviceIdType.MESH
F32 = jnp.float32
BF16 = jnp.bfloat16

CHUNKS = (
    (1, 0, 16, 0, 2),
    (2, 0, 16, 9, 2),
    (1, 16, 16, 0, 2),
    (2, 16, 16, 9, 2),
    (1, 0, 16, 2, 2),
    (1, 16, 16, 2, 2),
    (2, 0, 32, 11, 2),
    (1, 0, 32, 4, 2),
    (2, 0, 32, 13, 1),
    (1, 0, 32, 6, 2),
    (1, 0, 32, 8, 1),
    (2, 0, 32, 14, 1),
    (2, 0, 32, 15, 1),
)
PIECES = ((0, 2), (9, 2), (2, 2), (11, 2), (4, 2), (13, 1), (6, 2), (14, 1), (8, 1), (15, 1))

FAR_UP, FAR_DOWN, NEAR_UP, NEAR_DOWN, SUM_UP, SUM_DOWN, ACROSS = range(7)
FAR, SUMS, OVER = range(3)
ARRIVAL = (FAR, FAR, SUMS, SUMS, SUMS, SUMS, OVER)

PLAN = (
    ("m", 0), ("x", 0), ("e", 0), ("m", 1), ("y", 1), ("m", 4), ("e", 4), ("x", 4), ("m", 3),
    ("y", 3), ("d", 0), ("m", 5), ("x", 5), ("e", 5), ("m", 2), ("e", 2), ("x", 2), ("m", 7),
    ("e", 7), ("m", 8), ("y", 8), ("s", 1), ("m", 6), ("m", 9), ("m", 11), ("x", 9), ("d", 2),
    ("y", 6), ("d", 4), ("x", 7), ("e", 9), ("m", 12), ("y", 12), ("m", 10), ("x", 10),
    ("e", 10), ("y", 11), ("d", 5), ("s", 3), ("d", 7), ("d", 10), ("d", 9), ("s", 8), ("s", 6),
    ("s", 12), ("z", 7), ("z", 4), ("s", 11), ("z", 5), ("e", 1), ("e", 12), ("z", 0), ("d", 3),
    ("e", 3), ("d", 1), ("e", 6), ("z", 10), ("d", 8), ("z", 9), ("e", 8), ("d", 12), ("d", 6),
    ("e", 11), ("z", 2), ("d", 11), ("f", 0), ("f", 3), ("f", 5), ("f", 4), ("f", 7), ("f", 8),
    ("f", 10), ("f", 1), ("f", 9), ("f", 6), ("f", 12), ("f", 2), ("f", 11),
)


def kernel(
    dp_half,
    lengths_hbm,
    q_hbm,
    kv_hbm,
    res_hbm,
    w_hbm,
    hid,
    total_0,
    total_1,
    scale,
    lengths,
    q,
    kv,
    res,
    w,
    stage,
    att,
    part,
    far_up,
    far_down,
    from_down,
    from_up,
    across,
    len_sem,
    res_sem,
    q_sem,
    kv_sem,
    w_sem,
    swap_sem,
    a_send,
    a_recv,
    r_send,
    r_recv,
):
    seqs = q.shape[0]
    width = part.shape[3]
    unit = width // 16
    dp, tp = lax.axis_index("dp"), lax.axis_index("tp")
    y_hi, x, core = tp // 8, (tp // 2) % 4, tp % 2

    def peer(dx, dy):
        return (
            (dp + dy * dp_half) % (2 * dp_half),
            ((y_hi + dy) % 2) * 8 + ((x + dx) % 4) * 2 + core,
        )

    sibling = (dp, tp + 1 - 2 * core)

    def turn(i):
        h = i % 4
        return (2 - h * (h + 1) // 2) % 4, 1 - i // 4

    def kv_head(i):
        dx, dy = turn(i)
        return ((y_hi + dy) % 2) * 4 + (x + dx) % 4

    def q_copy(s, i, group):
        wide = GROUP * HEAD_DIM
        cols = pl.ds(pl.multiple_of(kv_head(i) * wide, wide), wide)
        return pltpu.make_async_copy(q_hbm.at[s, :, cols], q.at[s, i], q_sem.at[s, group])

    def kv_copy(s, i, group):
        return pltpu.make_async_copy(kv_hbm.at[s, kv_head(i)], kv.at[s, i], kv_sem.at[s, group])

    def w_copy(j):
        cols = pl.ds(PIECES[j][0] * unit, PIECES[j][1] * unit)
        return pltpu.make_async_copy(w_hbm.at[:, cols], w.at[0, :, cols], w_sem.at[j])

    def swap_copy(j):
        cols = pl.ds(PIECES[j][0] * unit, PIECES[j][1] * unit)
        return pltpu.make_async_remote_copy(
            w_hbm.at[:, cols],
            w.at[1, :, cols],
            swap_sem,
            w_sem.at[j],
            device_id=sibling,
            device_id_type=MESH,
        )

    def load_heads(s, count):
        for i in range(KV_HEADS):
            q_copy(s, i, i // count).start()
            kv_copy(s, i, i // count).start()

    def arrive(ref, sem):
        pltpu.make_async_copy(ref, ref, sem).wait()

    barrier = pltpu.get_barrier_semaphore()
    friends = [sibling] + [peer(i % 4, i // 4) for i in range(1, 8)]
    for friend in friends:
        pl.semaphore_signal(barrier, inc=1, device_id=friend, device_id_type=MESH)
    len_copy = pltpu.make_async_copy(lengths_hbm, lengths, len_sem)
    len_copy.start()
    load_heads(0, 2)
    res_copy = pltpu.make_async_copy(res_hbm, res, res_sem)

    def att_copy(s, i):
        dx, dy = turn(i)
        return pltpu.make_async_remote_copy(
            stage.at[s, i],
            att.at[dy, (4 - dx) % 4, pl.ds(s * DRAFT, DRAFT)],
            a_send,
            a_recv.at[s],
            device_id=peer(dx, dy),
            device_id_type=MESH,
        )

    slots = kv.shape[3 - 1]
    draft = lax.broadcasted_iota(jnp.int32, (GROUP * DRAFT, slots), 0) % DRAFT
    slot = lax.broadcasted_iota(jnp.int32, (GROUP * DRAFT, slots), 1)
    ahead = slot - draft

    def attend(s, heads, group):
        these = pl.ds(heads[0], len(heads))
        arrive(q.at[s, these], q_sem.at[s, group])
        arrive(kv.at[s, these], kv_sem.at[s, group])
        for i in heads:
            own = q[s, i]
            grouped = jnp.concatenate(
                [own[:, g * HEAD_DIM : (g + 1) * HEAD_DIM] for g in range(GROUP)], axis=0
            )
            keys = kv[s, i, :, :HEAD_DIM]
            values = kv[s, i, :, HEAD_DIM:]
            scores = lax.dot_general(
                grouped, keys, (((1,), (1,)), ((), ())), preferred_element_type=F32
            ) * (HEAD_DIM ** (-0.5))
            scores = jnp.where(ahead < lengths[s] - DRAFT + 1, scores, -1e30)
            raised = jnp.exp(scores - jnp.max(scores, axis=-1, keepdims=True))
            sums = jnp.sum(raised, axis=-1, keepdims=True)
            out = jnp.dot(raised.astype(BF16), values, preferred_element_type=F32)
            out = (out / sums).astype(BF16)
            stage[s, i] = jnp.concatenate(
                [out[g * DRAFT : (g + 1) * DRAFT] for g in range(GROUP)], axis=1
            )

    def some_heads(s, count):
        def body(h, carry):
            heads = [count * h + n for n in range(count)]
            attend(s, heads, h)
            for n in range(count - 1):
                att_copy(s, heads[n]).start()

            @pl.when(h < KV_HEADS // count - 1)
            def _():
                att_copy(s, heads[count - 1]).start()

            return carry

        return body

    with jax.named_scope("heads#s=0a"):
        len_copy.wait()
        attend(0, (0, 1), 0)
    for s in range(1, seqs):
        load_heads(s, 4)
    with jax.named_scope("barrier"):
        pl.semaphore_wait(barrier, len(friends))
    for i in (0, 1):
        att_copy(0, i).start()
    for j in range(len(PIECES)):
        swap_copy(j).start()
        w_copy(j).start()
    res_copy.start()
    with jax.named_scope("heads#s=0"):
        lax.fori_loop(1, KV_HEADS // 2, some_heads(0, 2), 0)
    for s in range(1, seqs):
        with jax.named_scope("heads#s=1"):
            lax.fori_loop(0, KV_HEADS // 4, some_heads(s, 4), 0)
    for s in range(seqs):
        att[0, 0, s * DRAFT : (s + 1) * DRAFT] = stage[s, KV_HEADS - 1]

    up, down, over = peer(1, 0), peer(3, 0), peer(0, 1)

    def area(c):
        kind, row, count, begin, size = CHUNKS[c]
        return kind, slice(row, row + count), slice(begin * unit, (begin + size) * unit)

    def halves(c):
        kind, row, count, begin, size = CHUNKS[c]
        mid, low, high = (begin * unit + size * unit // 2), begin * unit, (begin + size) * unit
        if count == seqs * DRAFT:
            half = count // 2
            return (slice(0, half), slice(low, high)), (slice(half, count), slice(low, high))
        lines = slice(row, row + count)
        return (lines, slice(low, mid)), (lines, slice(mid, high))

    def copies(c):
        kind, lines, cols = area(c)
        if kind == 1:
            pairs = {
                FAR_UP: (part.at[0, 2, lines, cols], far_up.at[lines, cols], up),
                FAR_DOWN: (part.at[1, 2, lines, cols], far_down.at[lines, cols], down),
                NEAR_UP: (part.at[1, 1, lines, cols], from_down.at[1, lines, cols], up),
                NEAR_DOWN: (part.at[0, 3, lines, cols], from_up.at[0, lines, cols], down),
                SUM_UP: (part.at[0, 1, lines, cols], from_down.at[0, lines, cols], up),
                SUM_DOWN: (part.at[1, 3, lines, cols], from_up.at[1, lines, cols], down),
                ACROSS: (part.at[1, 0, lines, cols], across.at[0, lines, cols], over),
            }
        else:
            one, two = halves(c)
            pairs = {
                FAR_UP: (part.at[0, 2, *one], far_up.at[*one], up),
                FAR_DOWN: (part.at[0, 2, *two], far_down.at[*two], down),
                NEAR_UP: (part.at[0, 1, *two], from_down.at[0, *two], up),
                NEAR_DOWN: (part.at[0, 3, *one], from_up.at[0, *one], down),
                SUM_UP: (part.at[0, 1, *one], from_down.at[0, *one], up),
                SUM_DOWN: (part.at[0, 3, *two], from_up.at[0, *two], down),
                ACROSS: (part.at[1, :, lines, cols], across.at[:, lines, cols], over),
            }

        def build(which):
            source, target, device = pairs[which]
            return pltpu.make_async_remote_copy(
                source,
                target,
                r_send,
                r_recv.at[c, ARRIVAL[which]],
                device_id=device,
                device_id_type=MESH,
            )

        return build

    def add(target, *terms):
        value = part[target].astype(F32)
        for ref, index in terms:
            value = value + ref[index].astype(F32)
        part[target] = value.astype(BF16)

    def wait_for(c, what):
        kind, lines, cols = area(c)
        one, two, four = far_up.at[lines, cols], from_down.at[:, lines, cols], across.at[:, lines, cols]
        sizes = {FAR: (two, one), SUMS: (four, two), OVER: (one, four)}
        arrive(sizes[what][kind - 1], r_recv.at[c, what])

    arrived, loaded = set(), set()
    squares = [0.0] * seqs

    def product(c):
        kind, row, count, begin, size = CHUNKS[c]
        for s in range(row // DRAFT, (row + count) // DRAFT):
            if s not in arrived:
                arrived.add(s)
                arrive(stage.at[s, : KV_HEADS - 1], a_recv.at[s])
        for j, (first, extent) in enumerate(PIECES):
            if j not in loaded and first < begin + size and begin < first + extent:
                loaded.add(j)
                arrive(w.at[:, :, first * unit : (first + extent) * unit], w_sem.at[j])

        def tile(n, carry):
            cols = pl.ds(pl.multiple_of(begin * unit + n * TILE, TILE), TILE)
            half = w.shape[1]
            own = pl.ds(pl.multiple_of(core * half, half), half)
            other = pl.ds(pl.multiple_of((1 - core) * half, half), half)
            lines = slice(row, row + count)
            out = jnp.dot(
                att[:, :, lines, own].reshape(8 * count, half),
                w[0, :, cols],
                preferred_element_type=F32,
            ) + jnp.dot(
                att[:, :, lines, other].reshape(8 * count, half),
                w[1, :, cols],
                preferred_element_type=F32,
            )
            part[:, :, lines, cols] = out.astype(BF16).reshape(2, 4, count, TILE)
            return carry

        lax.fori_loop(0, size * unit // TILE, tile, 0)

    def finish(c):
        kind, lines, cols = area(c)
        value = (
            part[0, 0, lines, cols].astype(F32)
            + from_down[0, lines, cols].astype(F32)
            + from_up[0, lines, cols].astype(F32)
            + across[0, lines, cols].astype(F32)
        )
        for n, s in enumerate(range(lines.start // DRAFT, lines.stop // DRAFT)):
            here = value[n * DRAFT : (n + 1) * DRAFT] + res[s, :, cols].astype(F32)
            (total_0, total_1)[s][:, cols] = here
            hid[s, :, cols] = here.astype(BF16)
            squares[s] = squares[s] + jnp.sum(here * here, axis=-1, keepdims=True)

    def advance(step, c):
        kind, lines, cols = area(c)
        build = copies(c)
        every = slice(None)
        if step == "m":
            product(c)
        elif step == "x":
            build(FAR_UP).start()
            build(FAR_DOWN).start()
        elif step == "e":
            build(NEAR_UP).start()
            build(NEAR_DOWN).start()
        elif step == "y":
            build(ACROSS).start()
        elif step == "s":
            wait_for(c, OVER)
            add((0, 2, lines, cols), (across, (2, lines, cols)))
            build(FAR_UP).start()
            build(FAR_DOWN).start()
            for dx in (1, 3):
                add((0, dx, lines, cols), (across, (dx, lines, cols)))
        elif step == "d":
            one, two = halves(c) if kind == 2 else ((lines, cols), (lines, cols))
            wait_for(c, FAR)
            add((0, 1, *one), (far_up, one))
            build(SUM_UP).start()
            add((0 if kind == 2 else 1, 3, *two), (far_down, two))
            build(SUM_DOWN).start()
        elif step == "z":
            wait_for(c, SUMS)
            add((1, 0, lines, cols), (from_down, (1, lines, cols)), (from_up, (1, lines, cols)))
            build(ACROSS).start()
        else:
            wait_for(c, OVER if kind == 1 else SUMS)
            finish(c)

    res_copy.wait()
    for step, c in PLAN:
        with jax.named_scope(f"{step}#c={c}"):
            advance(step, c)

    with jax.named_scope("scale"):
        for s in range(seqs):
            lane = lax.rsqrt(squares[s] / width + 1e-5)
            scale[s * DRAFT : (s + 1) * DRAFT, :] = jnp.broadcast_to(lane, (DRAFT, 128))

    with jax.named_scope("drain"):
        arrive(stage.at[:, : KV_HEADS - 1], a_send)
        arrive(w.at[0], swap_sem)
        sent = 0
        for kind, row, count, begin, size in CHUNKS:
            sent += (7 * count if kind == 1 else 3 * count + 4 * count) * size * unit
        arrive(w.at[0, :, : sent // w.shape[1]], r_send)


def norm_kernel(hid, total_0, total_1, scale, gain, hid_hbm, norm_hbm, norm, sems):
    hid_copy = pltpu.make_async_copy(hid, hid_hbm, sems.at[0])
    hid_copy.start()
    seqs, width = norm.shape[0], norm.shape[2]
    pieces = 4
    size = width // pieces

    def norm_copy(n):
        cols = pl.ds(n * size, size)
        return pltpu.make_async_copy(
            norm.at[:, :, cols], norm_hbm.at[:, :, cols], sems.at[1 + n]
        )

    for n in range(pieces):
        cols = slice(n * size, (n + 1) * size)
        gains = gain[cols].astype(F32).reshape(1, size)
        for s, total in enumerate((total_0, total_1)):
            lane = scale[s * DRAFT : (s + 1) * DRAFT, 0:1]
            norm[s, :, cols] = (total[:, cols] * lane * gains).astype(BF16)
        norm_copy(n).start()
    hid_copy.wait()
    for n in range(pieces):
        norm_copy(n).wait()


def solution(mesh):
    dp_half = mesh.shape["dp"] // 2

    def on_device(queries, kv_cache, lengths, residual, out_weight, norm_gain):
        seqs = queries.shape[0]
        rows = seqs * DRAFT
        depth, width = out_weight.shape
        slots = kv_cache.shape[2]
        chunks, pieces = len(CHUNKS), len(PIECES)
        hbm = pl.BlockSpec(memory_space=pltpu.HBM)
        vmem = pl.BlockSpec(memory_space=pltpu.VMEM)
        dma = pltpu.SemaphoreType.DMA
        sums = pl.pallas_call(
            functools.partial(kernel, dp_half),
            out_shape=(
                jax.ShapeDtypeStruct((seqs, DRAFT, width), BF16),
                jax.ShapeDtypeStruct((DRAFT, width), F32),
                jax.ShapeDtypeStruct((DRAFT, width), F32),
                jax.ShapeDtypeStruct((rows, 128), F32),
            ),
            in_specs=[pl.BlockSpec(memory_space=pl.ANY)] + [hbm] * 4,
            out_specs=(vmem,) * 4,
            scratch_shapes=[
                pltpu.SMEM((seqs,), jnp.int32),
                pltpu.VMEM((seqs, KV_HEADS, DRAFT, GROUP * HEAD_DIM), BF16),
                pltpu.VMEM((seqs, KV_HEADS, slots, 2 * HEAD_DIM), BF16),
                pltpu.VMEM(residual.shape, BF16),
                pltpu.VMEM((2, depth, width), BF16),
                pltpu.VMEM((seqs, KV_HEADS, DRAFT, GROUP * HEAD_DIM), BF16),
                pltpu.VMEM((2, 4, rows, GROUP * HEAD_DIM), BF16),
                pltpu.VMEM((2, 4, rows, width), BF16),
                pltpu.VMEM((rows, width), BF16),
                pltpu.VMEM((rows, width), BF16),
                pltpu.VMEM((2, rows, width), BF16),
                pltpu.VMEM((2, rows, width), BF16),
                pltpu.VMEM((4, rows, width), BF16),
                dma,
                dma,
                dma((seqs, KV_HEADS // 2)),
                dma((seqs, KV_HEADS // 2)),
                dma((pieces,)),
                dma,
                dma,
                dma((seqs,)),
                dma,
                dma((chunks, 3)),
            ],
            compiler_params=pltpu.CompilerParams(
                collective_id=0, has_side_effects=True, vmem_limit_bytes=VMEM_LIMIT
            ),
        )(lengths, queries, kv_cache, residual, out_weight)
        return pl.pallas_call(
            norm_kernel,
            out_shape=(jax.ShapeDtypeStruct((seqs, DRAFT, width), BF16),) * 2,
            in_specs=[vmem] * 5,
            out_specs=(hbm, hbm),
            scratch_shapes=[pltpu.VMEM((seqs, DRAFT, width), BF16), dma((5,))],
            compiler_params=pltpu.CompilerParams(vmem_limit_bytes=4 * 1024 * 1024),
        )(*sums, norm_gain)

    seq = P(("dp", "tp"))
    return jax.shard_map(
        on_device,
        mesh=mesh,
        in_specs=(seq, seq, seq, seq, P("tp"), P()),
        out_specs=(seq, seq),
        check_vma=False,
    )
```

```python
import functools

import jax
import jax.numpy as jnp
from jax import lax
from jax.experimental import pallas as pl
from jax.experimental.pallas import tpu as pltpu
from jax.sharding import PartitionSpec as P

KV_HEADS = 8
HEAD_DIM = 128
GROUP = 8
DRAFT = 16
TILE = 512
VMEM_LIMIT = 50 * 1024 * 1024
MESH = pl.DeviceIdType.MESH
F32 = jnp.float32
BF16 = jnp.bfloat16

CHUNKS = (
    (1, 0, 16, 0, 2),
    (2, 0, 16, 9, 2),
    (1, 16, 16, 0, 2),
    (2, 16, 16, 9, 2),
    (1, 0, 16, 2, 2),
    (1, 16, 16, 2, 2),
    (2, 0, 32, 11, 2),
    (1, 0, 32, 4, 2),
    (2, 0, 32, 13, 1),
    (1, 0, 32, 6, 2),
    (1, 0, 32, 8, 1),
    (2, 0, 32, 14, 1),
    (2, 0, 32, 15, 1),
)
PIECES = ((0, 2), (9, 2), (2, 2), (11, 2), (4, 2), (13, 1), (6, 2), (14, 1), (8, 1), (15, 1))

FAR_UP, FAR_DOWN, NEAR_UP, NEAR_DOWN, SUM_UP, SUM_DOWN, ACROSS = range(7)
FAR, SUMS, OVER = range(3)
ARRIVAL = (FAR, FAR, SUMS, SUMS, SUMS, SUMS, OVER)

PLAN = (
    ("m", 0), ("x", 0), ("m", 1), ("y", 1), ("e", 0), ("m", 4), ("e", 4), ("x", 4), ("m", 3),
    ("y", 3), ("d", 0), ("m", 2), ("x", 2), ("e", 2), ("m", 5), ("x", 5), ("m", 8), ("y", 8),
    ("e", 5), ("m", 7), ("e", 7), ("m", 6), ("y", 6), ("d", 2), ("m", 9), ("x", 7), ("m", 10),
    ("x", 9), ("e", 10), ("m", 11), ("x", 10), ("s", 8), ("s", 1), ("e", 9), ("y", 11),
    ("e", 1), ("d", 5), ("s", 3), ("d", 9), ("d", 10), ("d", 4), ("m", 12), ("y", 12), ("d", 7),
    ("s", 6), ("s", 11), ("z", 9), ("d", 3), ("z", 2), ("z", 0), ("d", 1), ("s", 12), ("d", 8),
    ("e", 3), ("e", 8), ("z", 7), ("z", 5), ("z", 4), ("d", 11), ("e", 11), ("d", 6), ("e", 6),
    ("z", 10), ("f", 9), ("e", 12), ("d", 12), ("f", 2), ("f", 0), ("f", 8), ("f", 1), ("f", 7),
    ("f", 4), ("f", 3), ("f", 5), ("f", 11), ("f", 10), ("f", 6), ("f", 12),
)


def kernel(
    dp_half,
    lengths_hbm,
    q_hbm,
    kv_hbm,
    res_hbm,
    w_hbm,
    hid,
    total_0,
    total_1,
    scale,
    lengths,
    q,
    kv,
    res,
    w,
    stage,
    att,
    part,
    far_up,
    far_down,
    from_down,
    from_up,
    across,
    len_sem,
    res_sem,
    q_sem,
    kv_sem,
    w_sem,
    swap_sem,
    a_send,
    a_recv,
    r_send,
    r_recv,
):
    seqs = q.shape[0]
    width = part.shape[3]
    unit = width // 16
    dp, tp = lax.axis_index("dp"), lax.axis_index("tp")
    y_hi, x, core = tp // 8, (tp // 2) % 4, tp % 2

    def peer(dx, dy):
        return (
            (dp + dy * dp_half) % (2 * dp_half),
            ((y_hi + dy) % 2) * 8 + ((x + dx) % 4) * 2 + core,
        )

    sibling = (dp, tp + 1 - 2 * core)

    def turn(i):
        h = i % 4
        return (2 - h * (h + 1) // 2) % 4, 1 - i // 4

    def kv_head(i):
        dx, dy = turn(i)
        return ((y_hi + dy) % 2) * 4 + (x + dx) % 4

    def q_copy(s, i, group):
        wide = GROUP * HEAD_DIM
        cols = pl.ds(pl.multiple_of(kv_head(i) * wide, wide), wide)
        return pltpu.make_async_copy(q_hbm.at[s, :, cols], q.at[s, i], q_sem.at[s, group])

    def kv_copy(s, i, group):
        return pltpu.make_async_copy(kv_hbm.at[s, kv_head(i)], kv.at[s, i], kv_sem.at[s, group])

    def w_copy(j):
        cols = pl.ds(PIECES[j][0] * unit, PIECES[j][1] * unit)
        return pltpu.make_async_copy(w_hbm.at[:, cols], w.at[0, :, cols], w_sem.at[j])

    def swap_copy(j):
        cols = pl.ds(PIECES[j][0] * unit, PIECES[j][1] * unit)
        return pltpu.make_async_remote_copy(
            w_hbm.at[:, cols],
            w.at[1, :, cols],
            swap_sem,
            w_sem.at[j],
            device_id=sibling,
            device_id_type=MESH,
        )

    def load_heads(s, count):
        for i in range(KV_HEADS):
            q_copy(s, i, i // count).start()
            kv_copy(s, i, i // count).start()

    def arrive(ref, sem):
        pltpu.make_async_copy(ref, ref, sem).wait()

    barrier = pltpu.get_barrier_semaphore()
    friends = [sibling] + [peer(i % 4, i // 4) for i in range(1, 8)]
    for friend in friends:
        pl.semaphore_signal(barrier, inc=1, device_id=friend, device_id_type=MESH)
    len_copy = pltpu.make_async_copy(lengths_hbm, lengths, len_sem)
    len_copy.start()
    load_heads(0, 2)
    res_copy = pltpu.make_async_copy(res_hbm, res, res_sem)

    def att_copy(s, i):
        dx, dy = turn(i)
        return pltpu.make_async_remote_copy(
            stage.at[s, i],
            att.at[dy, (4 - dx) % 4, pl.ds(s * DRAFT, DRAFT)],
            a_send,
            a_recv.at[s],
            device_id=peer(dx, dy),
            device_id_type=MESH,
        )

    slots = kv.shape[3 - 1]
    draft = lax.broadcasted_iota(jnp.int32, (GROUP * DRAFT, slots), 0) % DRAFT
    slot = lax.broadcasted_iota(jnp.int32, (GROUP * DRAFT, slots), 1)
    ahead = slot - draft

    def attend(s, heads, group):
        these = pl.ds(heads[0], len(heads))
        arrive(q.at[s, these], q_sem.at[s, group])
        arrive(kv.at[s, these], kv_sem.at[s, group])
        for i in heads:
            own = q[s, i]
            grouped = jnp.concatenate(
                [own[:, g * HEAD_DIM : (g + 1) * HEAD_DIM] for g in range(GROUP)], axis=0
            )
            keys = kv[s, i, :, :HEAD_DIM]
            values = kv[s, i, :, HEAD_DIM:]
            scores = lax.dot_general(
                grouped, keys, (((1,), (1,)), ((), ())), preferred_element_type=F32
            ) * (HEAD_DIM ** (-0.5))
            scores = jnp.where(ahead < lengths[s] - DRAFT + 1, scores, -1e30)
            raised = jnp.exp(scores - jnp.max(scores, axis=-1, keepdims=True))
            sums = jnp.sum(raised, axis=-1, keepdims=True)
            out = jnp.dot(raised.astype(BF16), values, preferred_element_type=F32)
            out = (out / sums).astype(BF16)
            stage[s, i] = jnp.concatenate(
                [out[g * DRAFT : (g + 1) * DRAFT] for g in range(GROUP)], axis=1
            )

    def some_heads(s, count):
        def body(h, carry):
            heads = [count * h + n for n in range(count)]
            attend(s, heads, h)
            for n in range(count - 1):
                att_copy(s, heads[n]).start()

            @pl.when(h < KV_HEADS // count - 1)
            def _():
                att_copy(s, heads[count - 1]).start()

            return carry

        return body

    with jax.named_scope("heads#s=0a"):
        len_copy.wait()
        attend(0, (0, 1), 0)
    for s in range(1, seqs):
        load_heads(s, 4)
    with jax.named_scope("barrier"):
        pl.semaphore_wait(barrier, len(friends))
    for i in (0, 1):
        att_copy(0, i).start()
    for j in range(len(PIECES)):
        swap_copy(j).start()
        w_copy(j).start()
    res_copy.start()
    with jax.named_scope("heads#s=0"):
        lax.fori_loop(1, KV_HEADS // 2, some_heads(0, 2), 0)
    for s in range(1, seqs):
        with jax.named_scope("heads#s=1"):
            lax.fori_loop(0, KV_HEADS // 4, some_heads(s, 4), 0)
    for s in range(seqs):
        att[0, 0, s * DRAFT : (s + 1) * DRAFT] = stage[s, KV_HEADS - 1]

    up, down, over = peer(1, 0), peer(3, 0), peer(0, 1)

    def area(c):
        kind, row, count, begin, size = CHUNKS[c]
        return kind, slice(row, row + count), slice(begin * unit, (begin + size) * unit)

    def halves(c):
        kind, row, count, begin, size = CHUNKS[c]
        mid, low, high = (begin * unit + size * unit // 2), begin * unit, (begin + size) * unit
        if count == seqs * DRAFT:
            half = count // 2
            return (slice(0, half), slice(low, high)), (slice(half, count), slice(low, high))
        lines = slice(row, row + count)
        return (lines, slice(low, mid)), (lines, slice(mid, high))

    def copies(c):
        kind, lines, cols = area(c)
        if kind == 1:
            pairs = {
                FAR_UP: (part.at[0, 2, lines, cols], far_up.at[lines, cols], up),
                FAR_DOWN: (part.at[1, 2, lines, cols], far_down.at[lines, cols], down),
                NEAR_UP: (part.at[1, 1, lines, cols], from_down.at[1, lines, cols], up),
                NEAR_DOWN: (part.at[0, 3, lines, cols], from_up.at[0, lines, cols], down),
                SUM_UP: (part.at[0, 1, lines, cols], from_down.at[0, lines, cols], up),
                SUM_DOWN: (part.at[1, 3, lines, cols], from_up.at[1, lines, cols], down),
                ACROSS: (part.at[1, 0, lines, cols], across.at[0, lines, cols], over),
            }
        else:
            one, two = halves(c)
            pairs = {
                FAR_UP: (part.at[0, 2, *one], far_up.at[*one], up),
                FAR_DOWN: (part.at[0, 2, *two], far_down.at[*two], down),
                NEAR_UP: (part.at[0, 1, *two], from_down.at[0, *two], up),
                NEAR_DOWN: (part.at[0, 3, *one], from_up.at[0, *one], down),
                SUM_UP: (part.at[0, 1, *one], from_down.at[0, *one], up),
                SUM_DOWN: (part.at[0, 3, *two], from_up.at[0, *two], down),
                ACROSS: (part.at[1, :, lines, cols], across.at[:, lines, cols], over),
            }

        def build(which):
            source, target, device = pairs[which]
            return pltpu.make_async_remote_copy(
                source,
                target,
                r_send,
                r_recv.at[c, ARRIVAL[which]],
                device_id=device,
                device_id_type=MESH,
            )

        return build

    def add(target, *terms):
        value = part[target].astype(F32)
        for ref, index in terms:
            value = value + ref[index].astype(F32)
        part[target] = value.astype(BF16)

    def wait_for(c, what):
        kind, lines, cols = area(c)
        one, two, four = far_up.at[lines, cols], from_down.at[:, lines, cols], across.at[:, lines, cols]
        sizes = {FAR: (two, one), SUMS: (four, two), OVER: (one, four)}
        arrive(sizes[what][kind - 1], r_recv.at[c, what])

    arrived, loaded = set(), set()
    squares = [0.0] * seqs

    def product(c):
        kind, row, count, begin, size = CHUNKS[c]
        for s in range(row // DRAFT, (row + count) // DRAFT):
            if s not in arrived:
                arrived.add(s)
                arrive(stage.at[s, : KV_HEADS - 1], a_recv.at[s])
        for j, (first, extent) in enumerate(PIECES):
            if j not in loaded and first < begin + size and begin < first + extent:
                loaded.add(j)
                arrive(w.at[:, :, first * unit : (first + extent) * unit], w_sem.at[j])

        def tile(n, carry):
            cols = pl.ds(pl.multiple_of(begin * unit + n * TILE, TILE), TILE)
            half = w.shape[1]
            own = pl.ds(pl.multiple_of(core * half, half), half)
            other = pl.ds(pl.multiple_of((1 - core) * half, half), half)
            lines = slice(row, row + count)
            out = jnp.dot(
                att[:, :, lines, own].reshape(8 * count, half),
                w[0, :, cols],
                preferred_element_type=F32,
            ) + jnp.dot(
                att[:, :, lines, other].reshape(8 * count, half),
                w[1, :, cols],
                preferred_element_type=F32,
            )
            part[:, :, lines, cols] = out.astype(BF16).reshape(2, 4, count, TILE)
            return carry

        lax.fori_loop(0, size * unit // TILE, tile, 0)

    def finish(c):
        kind, lines, cols = area(c)
        value = (
            part[0, 0, lines, cols].astype(F32)
            + from_down[0, lines, cols].astype(F32)
            + from_up[0, lines, cols].astype(F32)
            + across[0, lines, cols].astype(F32)
        )
        for n, s in enumerate(range(lines.start // DRAFT, lines.stop // DRAFT)):
            here = value[n * DRAFT : (n + 1) * DRAFT] + res[s, :, cols].astype(F32)
            (total_0, total_1)[s][:, cols] = here
            hid[s, :, cols] = here.astype(BF16)
            squares[s] = squares[s] + jnp.sum(here * here, axis=-1, keepdims=True)

    def advance(step, c):
        kind, lines, cols = area(c)
        build = copies(c)
        every = slice(None)
        if step == "m":
            product(c)
        elif step == "x":
            build(FAR_UP).start()
            build(FAR_DOWN).start()
        elif step == "e":
            build(NEAR_UP).start()
            build(NEAR_DOWN).start()
        elif step == "y":
            build(ACROSS).start()
        elif step == "s":
            wait_for(c, OVER)
            add((0, 2, lines, cols), (across, (2, lines, cols)))
            build(FAR_UP).start()
            build(FAR_DOWN).start()
            for dx in (1, 3):
                add((0, dx, lines, cols), (across, (dx, lines, cols)))
        elif step == "d":
            one, two = halves(c) if kind == 2 else ((lines, cols), (lines, cols))
            wait_for(c, FAR)
            add((0, 1, *one), (far_up, one))
            build(SUM_UP).start()
            add((0 if kind == 2 else 1, 3, *two), (far_down, two))
            build(SUM_DOWN).start()
        elif step == "z":
            wait_for(c, SUMS)
            add((1, 0, lines, cols), (from_down, (1, lines, cols)), (from_up, (1, lines, cols)))
            build(ACROSS).start()
        else:
            wait_for(c, OVER if kind == 1 else SUMS)
            finish(c)

    res_copy.wait()
    for step, c in PLAN:
        with jax.named_scope(f"{step}#c={c}"):
            advance(step, c)

    with jax.named_scope("scale"):
        for s in range(seqs):
            lane = lax.rsqrt(squares[s] / width + 1e-5)
            scale[s * DRAFT : (s + 1) * DRAFT, :] = jnp.broadcast_to(lane, (DRAFT, 128))

    with jax.named_scope("drain"):
        arrive(stage.at[:, : KV_HEADS - 1], a_send)
        arrive(w.at[0], swap_sem)
        sent = 0
        for kind, row, count, begin, size in CHUNKS:
            sent += (7 * count if kind == 1 else 3 * count + 4 * count) * size * unit
        arrive(w.at[0, :, : sent // w.shape[1]], r_send)


def norm_kernel(hid, total_0, total_1, scale, gain, hid_hbm, norm_hbm, norm, sems):
    hid_copy = pltpu.make_async_copy(hid, hid_hbm, sems.at[0])
    hid_copy.start()
    seqs, width = norm.shape[0], norm.shape[2]
    pieces = 4
    size = width // pieces

    def norm_copy(n):
        cols = pl.ds(n * size, size)
        return pltpu.make_async_copy(
            norm.at[:, :, cols], norm_hbm.at[:, :, cols], sems.at[1 + n]
        )

    for n in range(pieces):
        cols = slice(n * size, (n + 1) * size)
        gains = gain[cols].astype(F32).reshape(1, size)
        for s, total in enumerate((total_0, total_1)):
            lane = scale[s * DRAFT : (s + 1) * DRAFT, 0:1]
            norm[s, :, cols] = (total[:, cols] * lane * gains).astype(BF16)
        norm_copy(n).start()
    hid_copy.wait()
    for n in range(pieces):
        norm_copy(n).wait()


def solution(mesh):
    dp_half = mesh.shape["dp"] // 2

    def on_device(queries, kv_cache, lengths, residual, out_weight, norm_gain):
        seqs = queries.shape[0]
        rows = seqs * DRAFT
        depth, width = out_weight.shape
        slots = kv_cache.shape[2]
        chunks, pieces = len(CHUNKS), len(PIECES)
        hbm = pl.BlockSpec(memory_space=pltpu.HBM)
        vmem = pl.BlockSpec(memory_space=pltpu.VMEM)
        dma = pltpu.SemaphoreType.DMA
        in_hbm = functools.partial(pltpu.with_memory_space_constraint, memory_space=pltpu.HBM)
        sums = pl.pallas_call(
            functools.partial(kernel, dp_half),
            out_shape=(
                jax.ShapeDtypeStruct((seqs, DRAFT, width), BF16),
                jax.ShapeDtypeStruct((DRAFT, width), F32),
                jax.ShapeDtypeStruct((DRAFT, width), F32),
                jax.ShapeDtypeStruct((rows, 128), F32),
            ),
            in_specs=[hbm] * 5,
            out_specs=(vmem,) * 4,
            scratch_shapes=[
                pltpu.SMEM((seqs,), jnp.int32),
                pltpu.VMEM((seqs, KV_HEADS, DRAFT, GROUP * HEAD_DIM), BF16),
                pltpu.VMEM((seqs, KV_HEADS, slots, 2 * HEAD_DIM), BF16),
                pltpu.VMEM(residual.shape, BF16),
                pltpu.VMEM((2, depth, width), BF16),
                pltpu.VMEM((seqs, KV_HEADS, DRAFT, GROUP * HEAD_DIM), BF16),
                pltpu.VMEM((2, 4, rows, GROUP * HEAD_DIM), BF16),
                pltpu.VMEM((2, 4, rows, width), BF16),
                pltpu.VMEM((rows, width), BF16),
                pltpu.VMEM((rows, width), BF16),
                pltpu.VMEM((2, rows, width), BF16),
                pltpu.VMEM((2, rows, width), BF16),
                pltpu.VMEM((4, rows, width), BF16),
                dma,
                dma,
                dma((seqs, KV_HEADS // 2)),
                dma((seqs, KV_HEADS // 2)),
                dma((pieces,)),
                dma,
                dma,
                dma((seqs,)),
                dma,
                dma((chunks, 3)),
            ],
            compiler_params=pltpu.CompilerParams(
                collective_id=0, has_side_effects=True, vmem_limit_bytes=VMEM_LIMIT
            ),
        )(*(in_hbm(a) for a in (lengths, queries, kv_cache, residual, out_weight)))
        return pl.pallas_call(
            norm_kernel,
            out_shape=(jax.ShapeDtypeStruct((seqs, DRAFT, width), BF16),) * 2,
            in_specs=[vmem] * 5,
            out_specs=(hbm, hbm),
            scratch_shapes=[pltpu.VMEM((seqs, DRAFT, width), BF16), dma((5,))],
            compiler_params=pltpu.CompilerParams(vmem_limit_bytes=4 * 1024 * 1024),
        )(*sums, norm_gain)

    seq = P(("dp", "tp"))
    return jax.shard_map(
        on_device,
        mesh=mesh,
        in_specs=(seq, seq, seq, seq, P("tp"), P()),
        out_specs=(seq, seq),
        check_vma=False,
    )
```

```python
import functools

import jax
import jax.numpy as jnp
from jax import lax
from jax.experimental import pallas as pl
from jax.experimental.pallas import tpu as pltpu
from jax.sharding import PartitionSpec as P

KV_HEADS = 8
HEAD_DIM = 128
GROUP = 8
DRAFT = 16
TILE = 512
VMEM_LIMIT = 50 * 1024 * 1024
MESH = pl.DeviceIdType.MESH
F32 = jnp.float32
BF16 = jnp.bfloat16

CHUNKS = (
    (1, 0, 16, 0, 2),
    (2, 0, 16, 9, 2),
    (1, 16, 16, 0, 2),
    (2, 16, 16, 9, 2),
    (1, 0, 16, 2, 2),
    (1, 16, 16, 2, 2),
    (2, 0, 32, 11, 2),
    (1, 0, 32, 4, 2),
    (2, 0, 32, 13, 1),
    (1, 0, 32, 6, 2),
    (1, 0, 32, 8, 1),
    (2, 0, 32, 14, 1),
    (2, 0, 32, 15, 1),
)
PIECES = ((0, 2), (9, 2), (2, 2), (11, 2), (4, 2), (13, 1), (6, 2), (14, 1), (8, 1), (15, 1))

FAR_UP, FAR_DOWN, NEAR_UP, NEAR_DOWN, SUM_UP, SUM_DOWN, ACROSS = range(7)
FAR, SUMS, OVER = range(3)
ARRIVAL = (FAR, FAR, SUMS, SUMS, SUMS, SUMS, OVER)

PLAN_0 = (
    ("m", 0), ("e", 0), ("m", 1), ("x", 0), ("y", 1), ("m", 4), ("e", 4), ("x", 4), ("m", 5),
    ("x", 5), ("e", 5), ("m", 6), ("y", 6), ("m", 2), ("x", 2), ("d", 0), ("m", 7), ("x", 7),
    ("e", 7), ("m", 3), ("y", 3), ("m", 9), ("m", 11), ("m", 10), ("d", 4), ("s", 1), ("e", 9),
    ("e", 10), ("m", 8), ("x", 10), ("x", 9), ("y", 11), ("d", 5), ("z", 0), ("y", 8),
    ("m", 12), ("y", 12), ("s", 6), ("d", 7), ("e", 2), ("d", 2), ("s", 11), ("s", 8), ("d", 9),
    ("d", 10), ("s", 3), ("f", 0), ("z", 5), ("s", 12), ("d", 6), ("e", 12), ("e", 11),
    ("d", 8), ("z", 7), ("d", 1), ("e", 3), ("z", 2), ("e", 8), ("d", 11), ("e", 6), ("z", 10),
    ("d", 3), ("e", 1), ("z", 4), ("d", 12), ("z", 9), ("f", 4), ("f", 6), ("f", 10), ("f", 5),
    ("f", 2), ("f", 8), ("f", 3), ("f", 11), ("f", 7), ("f", 1), ("f", 12), ("f", 9),
)
PLAN_1 = (
    ("m", 0), ("x", 0), ("m", 1), ("y", 1), ("e", 0), ("m", 4), ("e", 4), ("x", 4), ("m", 3),
    ("d", 0), ("y", 3), ("m", 2), ("e", 2), ("x", 2), ("m", 5), ("x", 5), ("m", 7), ("x", 7),
    ("s", 1), ("m", 9), ("m", 11), ("e", 9), ("x", 9), ("m", 8), ("d", 5), ("y", 8), ("d", 4),
    ("s", 3), ("e", 7), ("m", 12), ("d", 2), ("d", 9), ("m", 10), ("m", 6), ("y", 6), ("e", 5),
    ("s", 8), ("y", 11), ("x", 10), ("y", 12), ("d", 10), ("e", 10), ("d", 7), ("s", 6),
    ("z", 9), ("s", 11), ("s", 12), ("d", 8), ("e", 6), ("e", 3), ("z", 2), ("d", 1), ("z", 0),
    ("e", 11), ("z", 5), ("z", 10), ("d", 3), ("z", 7), ("e", 1), ("e", 8), ("z", 4), ("d", 6),
    ("d", 11), ("e", 12), ("f", 9), ("d", 12), ("f", 2), ("f", 10), ("f", 5), ("f", 0),
    ("f", 8), ("f", 1), ("f", 3), ("f", 6), ("f", 11), ("f", 7), ("f", 4), ("f", 12),
)


def kernel(
    dp_half,
    lengths_hbm,
    q_hbm,
    kv_hbm,
    res_hbm,
    w_hbm,
    hid,
    total_0,
    total_1,
    scale,
    lengths,
    q,
    kv,
    res,
    w,
    stage,
    att,
    part,
    far_up,
    far_down,
    from_down,
    from_up,
    across,
    len_sem,
    res_sem,
    q_sem,
    kv_sem,
    w_sem,
    swap_sem,
    a_send,
    a_recv,
    r_send,
    r_recv,
):
    seqs = q.shape[0]
    width = part.shape[3]
    unit = width // 16
    dp, tp = lax.axis_index("dp"), lax.axis_index("tp")
    y_hi, x, core = tp // 8, (tp // 2) % 4, tp % 2

    def peer(dx, dy):
        return (
            (dp + dy * dp_half) % (2 * dp_half),
            ((y_hi + dy) % 2) * 8 + ((x + dx) % 4) * 2 + core,
        )

    sibling = (dp, tp + 1 - 2 * core)

    def turn(i):
        h = i % 4
        return (2 - h * (h + 1) // 2) % 4, 1 - i // 4

    def kv_head(i):
        dx, dy = turn(i)
        return ((y_hi + dy) % 2) * 4 + (x + dx) % 4

    def q_copy(s, i, group):
        wide = GROUP * HEAD_DIM
        cols = pl.ds(pl.multiple_of(kv_head(i) * wide, wide), wide)
        return pltpu.make_async_copy(q_hbm.at[s, :, cols], q.at[s, i], q_sem.at[s, group])

    def kv_copy(s, i, group):
        return pltpu.make_async_copy(kv_hbm.at[s, kv_head(i)], kv.at[s, i], kv_sem.at[s, group])

    def w_copy(j):
        cols = pl.ds(PIECES[j][0] * unit, PIECES[j][1] * unit)
        return pltpu.make_async_copy(w_hbm.at[:, cols], w.at[0, :, cols], w_sem.at[j])

    def swap_copy(j):
        cols = pl.ds(PIECES[j][0] * unit, PIECES[j][1] * unit)
        return pltpu.make_async_remote_copy(
            w_hbm.at[:, cols],
            w.at[1, :, cols],
            swap_sem,
            w_sem.at[j],
            device_id=sibling,
            device_id_type=MESH,
        )

    def load_heads(s, groups):
        for group, heads in enumerate(groups):
            for i in heads:
                q_copy(s, i, group).start()
                kv_copy(s, i, group).start()

    def arrive(ref, sem):
        pltpu.make_async_copy(ref, ref, sem).wait()

    barrier = pltpu.get_barrier_semaphore()
    friends = [sibling] + [peer(i % 4, i // 4) for i in range(1, 8)]
    for friend in friends:
        pl.semaphore_signal(barrier, inc=1, device_id=friend, device_id_type=MESH)
    len_copy = pltpu.make_async_copy(lengths_hbm, lengths, len_sem)
    len_copy.start()
    load_heads(0, ((0, 1), (2, 3), (4, 5), (6, 7)))
    res_copy = pltpu.make_async_copy(res_hbm, res, res_sem)

    def att_copy(s, i):
        dx, dy = turn(i)
        return pltpu.make_async_remote_copy(
            stage.at[s, i],
            att.at[dy, (4 - dx) % 4, pl.ds(s * DRAFT, DRAFT)],
            a_send,
            a_recv.at[s],
            device_id=peer(dx, dy),
            device_id_type=MESH,
        )

    slots = kv.shape[3 - 1]
    draft = lax.broadcasted_iota(jnp.int32, (GROUP * DRAFT, slots), 0) % DRAFT
    slot = lax.broadcasted_iota(jnp.int32, (GROUP * DRAFT, slots), 1)
    ahead = slot - draft

    def attend(s, heads, group):
        these = pl.ds(heads[0], len(heads))
        arrive(q.at[s, these], q_sem.at[s, group])
        arrive(kv.at[s, these], kv_sem.at[s, group])
        for i in heads:
            own = q[s, i]
            grouped = jnp.concatenate(
                [own[:, g * HEAD_DIM : (g + 1) * HEAD_DIM] for g in range(GROUP)], axis=0
            )
            keys = kv[s, i, :, :HEAD_DIM]
            values = kv[s, i, :, HEAD_DIM:]
            scores = lax.dot_general(
                grouped, keys, (((1,), (1,)), ((), ())), preferred_element_type=F32
            ) * (HEAD_DIM ** (-0.5))
            scores = jnp.where(ahead < lengths[s] - DRAFT + 1, scores, -1e30)
            raised = jnp.exp(scores - jnp.max(scores, axis=-1, keepdims=True))
            sums = jnp.sum(raised, axis=-1, keepdims=True)
            out = jnp.dot(raised.astype(BF16), values, preferred_element_type=F32)
            out = (out / sums).astype(BF16)
            stage[s, i] = jnp.concatenate(
                [out[g * DRAFT : (g + 1) * DRAFT] for g in range(GROUP)], axis=1
            )

    def some_heads(s, count):
        def body(h, carry):
            heads = [count * h + n for n in range(count)]
            attend(s, heads, h)
            for n in range(count - 1):
                att_copy(s, heads[n]).start()

            @pl.when(h < KV_HEADS // count - 1)
            def _():
                att_copy(s, heads[count - 1]).start()

            return carry

        return body

    with jax.named_scope("heads#s=0a"):
        len_copy.wait()
        attend(0, (0, 1), 0)
    for s in range(1, seqs):
        load_heads(s, ((0, 1), (2, 3), (4, 5, 6, 7)))
    with jax.named_scope("barrier"):
        pl.semaphore_wait(barrier, len(friends))
    for i in (0, 1):
        att_copy(0, i).start()
    for j in range(len(PIECES)):
        swap_copy(j).start()
        w_copy(j).start()
    res_copy.start()
    with jax.named_scope("heads#s=0"):
        lax.fori_loop(1, KV_HEADS // 2, some_heads(0, 2), 0)
    for s in range(1, seqs):
        with jax.named_scope("heads#s=1"):
            lax.fori_loop(0, 2, some_heads(s, 2), 0)
            attend(s, (4, 5, 6, 7), 2)
            for i in (4, 5, 6):
                att_copy(s, i).start()
    for s in range(seqs):
        att[0, 0, s * DRAFT : (s + 1) * DRAFT] = stage[s, KV_HEADS - 1]

    up, down, over = peer(1, 0), peer(3, 0), peer(0, 1)

    def area(c):
        kind, row, count, begin, size = CHUNKS[c]
        return kind, slice(row, row + count), slice(begin * unit, (begin + size) * unit)

    def halves(c):
        kind, row, count, begin, size = CHUNKS[c]
        mid, low, high = (begin * unit + size * unit // 2), begin * unit, (begin + size) * unit
        if count == seqs * DRAFT:
            half = count // 2
            return (slice(0, half), slice(low, high)), (slice(half, count), slice(low, high))
        lines = slice(row, row + count)
        return (lines, slice(low, mid)), (lines, slice(mid, high))

    def copies(c):
        kind, lines, cols = area(c)
        if kind == 1:
            pairs = {
                FAR_UP: (part.at[0, 2, lines, cols], far_up.at[lines, cols], up),
                FAR_DOWN: (part.at[1, 2, lines, cols], far_down.at[lines, cols], down),
                NEAR_UP: (part.at[1, 1, lines, cols], from_down.at[1, lines, cols], up),
                NEAR_DOWN: (part.at[0, 3, lines, cols], from_up.at[0, lines, cols], down),
                SUM_UP: (part.at[0, 1, lines, cols], from_down.at[0, lines, cols], up),
                SUM_DOWN: (part.at[1, 3, lines, cols], from_up.at[1, lines, cols], down),
                ACROSS: (part.at[1, 0, lines, cols], across.at[0, lines, cols], over),
            }
        else:
            one, two = halves(c)
            pairs = {
                FAR_UP: (part.at[0, 2, *one], far_up.at[*one], up),
                FAR_DOWN: (part.at[0, 2, *two], far_down.at[*two], down),
                NEAR_UP: (part.at[0, 1, *two], from_down.at[0, *two], up),
                NEAR_DOWN: (part.at[0, 3, *one], from_up.at[0, *one], down),
                SUM_UP: (part.at[0, 1, *one], from_down.at[0, *one], up),
                SUM_DOWN: (part.at[0, 3, *two], from_up.at[0, *two], down),
                ACROSS: (part.at[1, :, lines, cols], across.at[:, lines, cols], over),
            }

        def build(which):
            source, target, device = pairs[which]
            return pltpu.make_async_remote_copy(
                source,
                target,
                r_send,
                r_recv.at[c, ARRIVAL[which]],
                device_id=device,
                device_id_type=MESH,
            )

        return build

    def add(target, *terms):
        value = part[target].astype(F32)
        for ref, index in terms:
            value = value + ref[index].astype(F32)
        part[target] = value.astype(BF16)

    def wait_for(c, what):
        kind, lines, cols = area(c)
        one, two, four = far_up.at[lines, cols], from_down.at[:, lines, cols], across.at[:, lines, cols]
        sizes = {FAR: (two, one), SUMS: (four, two), OVER: (one, four)}
        arrive(sizes[what][kind - 1], r_recv.at[c, what])

    def run(plan):
        arrived, loaded = set(), set()
        squares = [0.0] * seqs

        def product(c):
            kind, row, count, begin, size = CHUNKS[c]
            for s in range(row // DRAFT, (row + count) // DRAFT):
                if s not in arrived:
                    arrived.add(s)
                    arrive(stage.at[s, : KV_HEADS - 1], a_recv.at[s])
            for j, (first, extent) in enumerate(PIECES):
                if j not in loaded and first < begin + size and begin < first + extent:
                    loaded.add(j)
                    arrive(w.at[:, :, first * unit : (first + extent) * unit], w_sem.at[j])

            def tile(n, carry):
                cols = pl.ds(pl.multiple_of(begin * unit + n * TILE, TILE), TILE)
                half = w.shape[1]
                own = pl.ds(pl.multiple_of(core * half, half), half)
                other = pl.ds(pl.multiple_of((1 - core) * half, half), half)
                lines = slice(row, row + count)
                out = jnp.dot(
                    att[:, :, lines, own].reshape(8 * count, half),
                    w[0, :, cols],
                    preferred_element_type=F32,
                ) + jnp.dot(
                    att[:, :, lines, other].reshape(8 * count, half),
                    w[1, :, cols],
                    preferred_element_type=F32,
                )
                part[:, :, lines, cols] = out.astype(BF16).reshape(2, 4, count, TILE)
                return carry

            lax.fori_loop(0, size * unit // TILE, tile, 0)

        def finish(c):
            kind, lines, cols = area(c)
            value = (
                part[0, 0, lines, cols].astype(F32)
                + from_down[0, lines, cols].astype(F32)
                + from_up[0, lines, cols].astype(F32)
                + across[0, lines, cols].astype(F32)
            )
            for n, s in enumerate(range(lines.start // DRAFT, lines.stop // DRAFT)):
                here = value[n * DRAFT : (n + 1) * DRAFT] + res[s, :, cols].astype(F32)
                (total_0, total_1)[s][:, cols] = here
                hid[s, :, cols] = here.astype(BF16)
                squares[s] = squares[s] + jnp.sum(here * here, axis=-1, keepdims=True)

        def advance(step, c):
            kind, lines, cols = area(c)
            build = copies(c)
            every = slice(None)
            if step == "m":
                product(c)
            elif step == "x":
                build(FAR_UP).start()
                build(FAR_DOWN).start()
            elif step == "e":
                build(NEAR_UP).start()
                build(NEAR_DOWN).start()
            elif step == "y":
                build(ACROSS).start()
            elif step == "s":
                wait_for(c, OVER)
                add((0, 2, lines, cols), (across, (2, lines, cols)))
                build(FAR_UP).start()
                build(FAR_DOWN).start()
                for dx in (1, 3):
                    add((0, dx, lines, cols), (across, (dx, lines, cols)))
            elif step == "d":
                one, two = halves(c) if kind == 2 else ((lines, cols), (lines, cols))
                wait_for(c, FAR)
                add((0, 1, *one), (far_up, one))
                build(SUM_UP).start()
                add((0 if kind == 2 else 1, 3, *two), (far_down, two))
                build(SUM_DOWN).start()
            elif step == "z":
                wait_for(c, SUMS)
                add((1, 0, lines, cols), (from_down, (1, lines, cols)), (from_up, (1, lines, cols)))
                build(ACROSS).start()
            else:
                wait_for(c, OVER if kind == 1 else SUMS)
                finish(c)

        res_copy.wait()
        for step, c in plan:
            with jax.named_scope(f"{step}#c={c}"):
                advance(step, c)

        with jax.named_scope("scale"):
            for s in range(seqs):
                lane = lax.rsqrt(squares[s] / width + 1e-5)
                scale[s * DRAFT : (s + 1) * DRAFT, :] = jnp.broadcast_to(lane, (DRAFT, 128))

    @pl.when(core == 0)
    def _():
        run(PLAN_0)

    @pl.when(core == 1)
    def _():
        run(PLAN_1)

    with jax.named_scope("drain"):
        arrive(stage.at[:, : KV_HEADS - 1], a_send)
        arrive(w.at[0], swap_sem)
        sent = 0
        for kind, row, count, begin, size in CHUNKS:
            sent += (7 * count if kind == 1 else 3 * count + 4 * count) * size * unit
        arrive(w.at[0, :, : sent // w.shape[1]], r_send)


def norm_kernel(hid, total_0, total_1, scale, gain, hid_hbm, norm_hbm, norm, sems):
    hid_copy = pltpu.make_async_copy(hid, hid_hbm, sems.at[0])
    hid_copy.start()
    seqs, width = norm.shape[0], norm.shape[2]
    pieces = 4
    size = width // pieces

    def norm_copy(n):
        cols = pl.ds(n * size, size)
        return pltpu.make_async_copy(
            norm.at[:, :, cols], norm_hbm.at[:, :, cols], sems.at[1 + n]
        )

    for n in range(pieces):
        cols = slice(n * size, (n + 1) * size)
        gains = gain[cols].astype(F32).reshape(1, size)
        for s, total in enumerate((total_0, total_1)):
            lane = scale[s * DRAFT : (s + 1) * DRAFT, 0:1]
            norm[s, :, cols] = (total[:, cols] * lane * gains).astype(BF16)
        norm_copy(n).start()
    hid_copy.wait()
    for n in range(pieces):
        norm_copy(n).wait()


def solution(mesh):
    dp_half = mesh.shape["dp"] // 2

    def on_device(queries, kv_cache, lengths, residual, out_weight, norm_gain):
        seqs = queries.shape[0]
        rows = seqs * DRAFT
        depth, width = out_weight.shape
        slots = kv_cache.shape[2]
        chunks, pieces = len(CHUNKS), len(PIECES)
        hbm = pl.BlockSpec(memory_space=pltpu.HBM)
        vmem = pl.BlockSpec(memory_space=pltpu.VMEM)
        dma = pltpu.SemaphoreType.DMA
        in_hbm = functools.partial(pltpu.with_memory_space_constraint, memory_space=pltpu.HBM)
        sums = pl.pallas_call(
            functools.partial(kernel, dp_half),
            out_shape=(
                jax.ShapeDtypeStruct((seqs, DRAFT, width), BF16),
                jax.ShapeDtypeStruct((DRAFT, width), F32),
                jax.ShapeDtypeStruct((DRAFT, width), F32),
                jax.ShapeDtypeStruct((rows, 128), F32),
            ),
            in_specs=[hbm] * 5,
            out_specs=(vmem,) * 4,
            scratch_shapes=[
                pltpu.SMEM((seqs,), jnp.int32),
                pltpu.VMEM((seqs, KV_HEADS, DRAFT, GROUP * HEAD_DIM), BF16),
                pltpu.VMEM((seqs, KV_HEADS, slots, 2 * HEAD_DIM), BF16),
                pltpu.VMEM(residual.shape, BF16),
                pltpu.VMEM((2, depth, width), BF16),
                pltpu.VMEM((seqs, KV_HEADS, DRAFT, GROUP * HEAD_DIM), BF16),
                pltpu.VMEM((2, 4, rows, GROUP * HEAD_DIM), BF16),
                pltpu.VMEM((2, 4, rows, width), BF16),
                pltpu.VMEM((rows, width), BF16),
                pltpu.VMEM((rows, width), BF16),
                pltpu.VMEM((2, rows, width), BF16),
                pltpu.VMEM((2, rows, width), BF16),
                pltpu.VMEM((4, rows, width), BF16),
                dma,
                dma,
                dma((seqs, KV_HEADS // 2)),
                dma((seqs, KV_HEADS // 2)),
                dma((pieces,)),
                dma,
                dma,
                dma((seqs,)),
                dma,
                dma((chunks, 3)),
            ],
            compiler_params=pltpu.CompilerParams(
                collective_id=0, has_side_effects=True, vmem_limit_bytes=VMEM_LIMIT
            ),
        )(*(in_hbm(a) for a in (lengths, queries, kv_cache, residual, out_weight)))
        return pl.pallas_call(
            norm_kernel,
            out_shape=(jax.ShapeDtypeStruct((seqs, DRAFT, width), BF16),) * 2,
            in_specs=[vmem] * 5,
            out_specs=(hbm, hbm),
            scratch_shapes=[pltpu.VMEM((seqs, DRAFT, width), BF16), dma((5,))],
            compiler_params=pltpu.CompilerParams(vmem_limit_bytes=4 * 1024 * 1024),
        )(*sums, norm_gain)

    seq = P(("dp", "tp"))
    return jax.shard_map(
        on_device,
        mesh=mesh,
        in_specs=(seq, seq, seq, seq, P("tp"), P()),
        out_specs=(seq, seq),
        check_vma=False,
    )
```
